32 devices in a mesh: site: 8 (over z, x), dom: 4 (over y, core).
Axes of the slice: x: 2, y: 2, z: 4, core: 2. Of those that a mesh axis runs over, the one named last changes fastest.
Arguments:
- top_partial: float32 [16, 61, 4, 8192], P(None, None, 'dom', 'site'), may hold values from 0.001 to 1
- bottom_partial: float32 [16, 61, 4, 8192], P(None, None, 'dom', 'site'), may hold values from 0.001 to 1
- left_vectors: float32 [256, 61, 61], P('dom'), may hold values from 0.05 to 1
- right_vectors: float32 [256, 61, 61], P('dom'), may hold values from 0.05 to 1
- decay_rates: float32 [256, 61], P('dom'), may hold values from 0.05 to 8
- state_weights: float32 [256, 61], P('dom'), may hold values from 0.002 to 0.05
- part_rates: float32 [256], P('dom'), may hold values from 0.3 to 3
- branch_lengths: float32 [1997], replicated, may hold values from 0.02 to 0.5
- pattern_weights: int32 [4, 8192], P('dom', 'site'), may hold values from 0 to 9
- block_partition: int32 [4, 64], P('dom', 'site'), may hold values from 0 to 255
- chosen_branches: int32 [16], replicated, may hold values from 0 to 1996, as said below
Outputs:
- site_loglik: float32 [16, 4, 8192], P(None, 'dom', 'site')
- part_derivs: float32 [2, 16, 256], P(None, None, 'dom')
- new_lengths: float32 [1997], replicated
The draws below stay inside these ranges and needn't reach their ends.
Inputs may be any that keep to these rules, and one draw needn't show every extreme that they name: `chosen_branches`: distinct branch numbers.
All inputs are finite; a program needn't handle non-finite values.
Results may differ from the reference program's by a relative error of at most 0.0003.
Values sent between devices are 32-bit elements; how exact they have to be, the bound alone decides.
A program may use at most 64 MiB of HBM per device.

```python
import math
import jax
import jax.numpy as jnp
import numpy as np
from jax import lax

STATES = 61
BR = 16
BLK = 128
TREE_BR = 1997
PARTS_SIZE = 256
SG = 8192
NBLK_G = 64
N_DOM = 4


def draw_chosen_branches(key, part):
    picked = jax.random.permutation(jax.random.fold_in(key, 17), TREE_BR)
    return picked[:BR].astype(jnp.int32)


def with_ends(result, key, low, top_value):
    spot = [jax.random.randint(jax.random.fold_in(key, axis), (), 0, length) for axis, length in enumerate(result.shape)]
    longest = result.shape.index(max(result.shape))
    next_to = spot[:longest] + [(spot[longest] + 1) % result.shape[longest]] + spot[longest + 1:]
    return result.at[tuple(spot)].set(low).at[tuple(next_to)].set(top_value)


def block_levels(own_key, dims, shards, least, high):
    def one(position, parts):
        draws = jax.random.uniform(jax.random.fold_in(jax.random.fold_in(own_key, 6), position), (parts,), jnp.float32, least / len(shards), high / len(shards))
        return jnp.repeat(jnp.exp(draws), dims[position] // parts).reshape((-1,) + (1,) * (len(dims) - position - 1))

    level = one(*shards[0])
    for cut in shards[1:]:
        level = level * one(*cut)
    return level


def cumulative_ranks(count, skew):
    loads = [(1 << 20) // math.isqrt(standing ** skew) + 1 for standing in range(1, count + 1)]
    scale = 1 + sum(loads) // (1 << 30)
    return np.cumsum(np.array([max(1, weight // scale) for weight in loads]))


def ranked(key, extent, amount, slope):
    grid = cumulative_ranks(amount, slope)
    ticket = jax.random.randint(jax.random.fold_in(key, 1), extent, 0, int(grid[amount - 1]))
    standing = jnp.searchsorted(jnp.asarray(grid, jnp.int32), ticket, side="right")
    return jax.random.permutation(jax.random.fold_in(key, 2), amount)[standing].astype(jnp.int32)


def setup_inputs(seed: int = 0) -> dict:
    splits = jax.random.split(jax.random.key(seed), 12)
    top_partial = jnp.clip(jnp.exp(math.log(1.0) - 6.9077552 * jax.random.uniform(splits[0], (BR, STATES, N_DOM, SG), jnp.float32) ** block_levels(splits[0], (BR, STATES, N_DOM, SG), ((2, 4), (3, 8)), -0.2, 0.2)), 0.001, 1.0)
    bottom_partial = jnp.clip(jnp.exp(math.log(1.0) - 6.9077552 * jax.random.uniform(splits[1], (BR, STATES, N_DOM, SG), jnp.float32) ** block_levels(splits[1], (BR, STATES, N_DOM, SG), ((2, 4), (3, 8)), -0.2, 0.2)), 0.001, 1.0)
    left_vectors = jnp.clip(0.05 + 0.95 * jax.random.uniform(splits[2], (PARTS_SIZE, STATES, STATES), jnp.float32) ** block_levels(splits[2], (PARTS_SIZE, STATES, STATES), ((0, 4),), -0.2, 0.2), 0.05, 1.0)
    right_vectors = jnp.clip(0.05 + 0.95 * jax.random.uniform(splits[3], (PARTS_SIZE, STATES, STATES), jnp.float32) ** block_levels(splits[3], (PARTS_SIZE, STATES, STATES), ((0, 4),), -0.2, 0.2), 0.05, 1.0)
    decay_rates = jnp.clip(jnp.exp(math.log(8.0) - 5.075174 * jax.random.uniform(splits[4], (PARTS_SIZE, STATES), jnp.float32) ** block_levels(splits[4], (PARTS_SIZE, STATES), ((0, 4),), -0.2, 0.2)), 0.05, 8.0)
    state_weights = jnp.clip(jnp.exp(math.log(0.05) - 3.218876 * jax.random.uniform(splits[5], (PARTS_SIZE, STATES), jnp.float32) ** block_levels(splits[5], (PARTS_SIZE, STATES), ((0, 4),), -0.2, 0.2)), 0.002, 0.05)
    part_rates = jnp.clip(jnp.exp(math.log(3.0) - 2.3025851 * jax.random.uniform(splits[6], (PARTS_SIZE,), jnp.float32) ** block_levels(splits[6], (PARTS_SIZE,), ((0, 4),), -0.2, 0.2)), 0.3, 3.0)
    branch_lengths = jnp.clip(jnp.exp(jax.random.uniform(splits[7], (TREE_BR,), jnp.float32, math.log(0.02), math.log(0.5))), 0.02, 0.5)
    pattern_weights = with_ends(jax.random.randint(splits[8], (N_DOM, SG), 0, 10), jax.random.fold_in(splits[8], 1), 0, 9).astype(jnp.int32)
    block_partition = with_ends(ranked(splits[9], (N_DOM, NBLK_G), PARTS_SIZE, 2), jax.random.fold_in(splits[9], 3), 0, PARTS_SIZE - 1).astype(jnp.int32)
    chosen_branches = draw_chosen_branches(jax.random.fold_in(splits[11], 71), 0)
    return {"top_partial": top_partial, "bottom_partial": bottom_partial, "left_vectors": left_vectors, "right_vectors": right_vectors, "decay_rates": decay_rates, "state_weights": state_weights, "part_rates": part_rates, "branch_lengths": branch_lengths, "pattern_weights": pattern_weights, "block_partition": block_partition, "chosen_branches": chosen_branches}


def project(upper, lower, vec_left, vec_right, state_w):
    scaled = upper * jnp.transpose(state_w)[None, :, :, None]
    lefts = jnp.einsum('binl,nik->bknl', scaled, vec_left, precision=lax.Precision.HIGHEST)
    rights = jnp.einsum('nkj,bjnl->bknl', vec_right, lower, precision=lax.Precision.HIGHEST)
    return lefts, rights


def finish(lefts, rights, exponent, times, weight_f):
    joint = lefts * rights
    expo = jnp.transpose(exponent)[None, :, :, None]
    decayed = joint * jnp.exp(expo * times[:, None, None, None])
    like_zero = jnp.sum(decayed, axis=1)
    like_one = jnp.sum(decayed * expo, axis=1)
    like_two = jnp.sum(decayed * expo * expo, axis=1)
    first = like_one / like_zero
    second = like_two / like_zero - first * first
    loglik = weight_f[None] * jnp.log(like_zero)
    sums = jnp.stack([jnp.sum(weight_f[None] * first, axis=-1), jnp.sum(weight_f[None] * second, axis=-1)])
    return loglik, sums


def reference(top_partial, bottom_partial, left_vectors, right_vectors, decay_rates, state_weights, part_rates, branch_lengths, pattern_weights, block_partition, chosen_branches):
    times = branch_lengths[chosen_branches]
    upper_all = jnp.moveaxis(top_partial, 2, 0)
    lower_all = jnp.moveaxis(bottom_partial, 2, 0)

    def one_group(items):
        upper, lower, weights_g, blocks = items
        nblocks = blocks.shape[0]
        upper = upper.reshape(BR, STATES, nblocks, BLK)
        lower = lower.reshape(BR, STATES, nblocks, BLK)
        vec_left = left_vectors[blocks]
        vec_right = right_vectors[blocks]
        exponent = -decay_rates[blocks] * part_rates[blocks][:, None]
        lefts, rights = project(upper, lower, vec_left, vec_right, state_weights[blocks])
        weight_f = weights_g.astype(jnp.float32).reshape(nblocks, BLK)
        loglik, sums = finish(lefts, rights, exponent, times, weight_f)
        onehot = (blocks[:, None] == jnp.arange(PARTS_SIZE, dtype=jnp.int32)[None, :]).astype(jnp.float32)
        part_sums = jnp.einsum('abn,np->abp', sums, onehot, precision=lax.Precision.HIGHEST)
        return loglik.reshape(BR, nblocks * BLK), part_sums

    logliks, part_all = lax.map(one_group, (upper_all, lower_all, pattern_weights, block_partition))
    site_loglik = jnp.moveaxis(logliks, 0, 1)
    part_derivs = jnp.sum(part_all, axis=0)
    totals = jnp.sum(part_derivs, axis=2)
    updated = times - totals[0] / totals[1]
    new_lengths = branch_lengths.at[chosen_branches].set(updated)
    return site_loglik, part_derivs, new_lengths
```

```python
import functools

import jax
import jax.numpy as jnp
from jax import lax
from jax.experimental import pallas as pl
from jax.experimental.pallas import tpu as pltpu
from jax.sharding import PartitionSpec as P

BLK = 128
MESH = pl.DeviceIdType.MESH
F32 = jnp.float32
LOG2E = 1.4426950408889634
BF16 = jnp.bfloat16


def round_up(value, unit):
    return (value + unit - 1) // unit * unit


def split(value):
    high = value.astype(BF16)
    return high, (value - high.astype(F32)).astype(BF16)


def thirds(value):
    high = value.astype(BF16)
    rest = value - high.astype(F32)
    middle = rest.astype(BF16)
    return high, middle, (rest - middle.astype(F32)).astype(BF16)


def settle(ref, sem):
    pltpu.make_async_copy(ref, ref, sem).wait()


def body(
    cfg,
    top_hbm, bottom_hbm, left_hbm, right_hbm,
    decay_hbm, weight_hbm, rate_hbm, lengths_hbm, chosen_hbm,
    pattern_hbm, blocks_hbm, row_hbm,
    loglik_ref, share_ref, new_ref,
    top_v, bottom_v, tables_v, req_v, req_s, mine, passed, got,
    top_x, bottom_x, like_v, parts_v, pay_v, pay_in, ids_v, hot_v, old_v, pick_v, row_v,
    modes_v, rate_s, lengths_s, chosen_s, pattern_ref, blocks_s, blocks_ref,
    load_sem, small_sem, gossip, req_send, req_recv, tab_send, near_recv, pass_recv, far_recv,
    ids_send, ids_recv, pay_send, pay_recv,
):
    doms, sites, inner, branches, states, nblk, owned, pad, group = cfg
    me = lax.axis_index("dom")
    spot = lax.axis_index("site")
    dom_bits = doms.bit_length() - 1
    outer = sites // inner
    near, far = lax.rem(spot, inner), spot // inner
    kinds = 2 * branches
    rows = nblk // group

    def at_site(x, z):
        return lax.rem(far + z, outer) * inner + lax.rem(near + x, inner)

    def greet(sem):
        @pl.when(far > 0)
        def _():
            pl.semaphore_signal(
                sem, inc=1, device_id={"site": spot - inner}, device_id_type=MESH
            )

        @pl.when(far < outer - 1)
        def _():
            pl.semaphore_signal(
                sem, inc=1, device_id={"site": spot + inner}, device_id_type=MESH
            )

        for x in range(1, inner):
            pl.semaphore_signal(
                sem, inc=1, device_id={"site": at_site(x, 0)}, device_id_type=MESH
            )
        for d in reversed(range(1, doms)):
            pl.semaphore_signal(sem, inc=1, device_id={"dom": me ^ d}, device_id_type=MESH)

    around = (
        doms - 1 + inner - 1 + jnp.where(far > 0, 1, 0) + jnp.where(far < outer - 1, 1, 0)
    )

    tables = [
        pltpu.make_async_copy(source, tables_v.at[i, :, pl.ds(0, owned), :], load_sem.at[0])
        for i, source in enumerate((left_hbm, right_hbm))
    ]
    tops = [
        pltpu.make_async_copy(
            top_hbm.at[:, :, n, :], top_v.at[n, :, pl.ds(0, states), :], load_sem.at[1]
        )
        for n in range(nblk)
    ]
    bottoms = [
        pltpu.make_async_copy(
            bottom_hbm.at[:, :, n, :], bottom_v.at[n, :, pl.ds(0, states), :], load_sem.at[2]
        )
        for n in range(nblk)
    ]
    modes = [
        pltpu.make_async_copy(source, modes_v.at[i], load_sem.at[3])
        for i, source in enumerate((decay_hbm, weight_hbm))
    ]
    small = [
        pltpu.make_async_copy(source, dest, small_sem.at[i])
        for i, (source, dest) in enumerate((
            (blocks_hbm, blocks_ref),
            (rate_hbm, rate_s),
            (blocks_hbm, blocks_s),
            (lengths_hbm, lengths_s),
            (chosen_hbm, chosen_s),
            (pattern_hbm, pattern_ref),
            (row_hbm, row_v),
        ))
    ]

    small[0].start()
    barrier = pltpu.get_barrier_semaphore()
    greet(barrier)
    for load in modes + tables + small[1:] + tops:
        load.start()
    req_v[0] = jnp.zeros((1, BLK), jnp.int32)
    for side in (top_v, bottom_v):
        for n in range(nblk):
            side[n, :, states:pad, :] = jnp.zeros((branches, pad - states, BLK), F32)
    mine[...] = jnp.zeros(mine.shape, F32)

    small[0].wait()
    req_v[0, 0:1, 0:nblk] = blocks_ref[...]
    pl.semaphore_wait(barrier, around)

    for kind, dest in enumerate((req_s, req_v)):
        for delta in reversed(range(1, doms)):
            pltpu.make_async_remote_copy(
                src_ref=req_v.at[0],
                dst_ref=dest.at[delta],
                send_sem=req_send.at[kind],
                recv_sem=req_recv.at[kind],
                device_id={"dom": me ^ delta},
                device_id_type=MESH,
            ).start()
    greet(gossip.at[0])

    def convert(source, dest):
        def step(n, carry):
            for b in range(branches):
                high, low = split(source[n, b])
                at = n * (branches // 2) + b // 2
                lanes = (b % 2) * BLK
                dest[at, 0:pad, lanes:lanes + BLK] = high
                dest[at, pad:2 * pad, lanes:lanes + BLK] = low
            return carry

        lax.fori_loop(0, nblk, step, 0)

    settle(top_v.at[:, :, pl.ds(0, states), :], load_sem.at[1])
    for load in bottoms:
        load.start()
    convert(top_v, top_x)
    settle(modes_v, load_sem.at[3])
    settle(tables_v.at[:, :, pl.ds(0, owned), :], load_sem.at[0])
    for load in small[1:]:
        load.wait()
    settle(req_s.at[pl.ds(1, doms - 1)], req_recv.at[0])

    def gather(delta, n):
        wanted = blocks_s[0, n] if delta == 0 else req_s[delta, 0, n]
        relative = wanted - me * owned
        inside = jnp.logical_and(relative >= 0, relative < owned)
        keep = jnp.where(inside, 1.0, 0.0).astype(F32)
        p = jnp.clip(relative, 0, owned - 1)
        mine[delta, n, 0:states, 0:states] = tables_v[0, :, p, :] * keep
        mine[delta, n, 0:states, pad:pad + states] = tables_v[1, :, p, :] * keep
        rate = rate_s[p] * keep
        mine[delta, n, states:states + 1, pad:pad + states] = -modes_v[0, pl.ds(p, 1), :] * rate
        mine[delta, n, states + 1:states + 2, pad:pad + states] = (
            modes_v[1, pl.ds(p, 1), :] * keep
        )

    def send(bit, d, n):
        to = d ^ (1 << bit)
        if bit == 0:
            arrived = near_recv.at[0] if to == 0 else pass_recv.at[to, n]
        else:
            arrived = far_recv.at[bit, n] if to == 0 else pass_recv.at[to, n]
        return pltpu.make_async_remote_copy(
            src_ref=(mine if bit == 0 else passed).at[d, n],
            dst_ref=got.at[bit, to, n],
            send_sem=tab_send.at[d],
            recv_sem=arrived,
            device_id={"dom": me ^ (1 << bit)},
            device_id_type=MESH,
        )

    def forward(bit, d, n):
        total = mine[d, n]
        for earlier in range(bit):
            send(earlier, d | (1 << earlier), n).wait_recv()
            total = total + got[earlier, d, n]
        passed[d, n] = total
        send(bit, d, n).start()

    for d in reversed(range(2, doms)):
        if d & 1:
            for n in range(nblk):
                gather(d, n)
                send(0, d, n).start()
    for d in reversed(range(2, doms)):
        if not d & 1:
            for n in range(nblk):
                gather(d, n)
    for bit in range(1, dom_bits):
        for d in reversed(range(doms)):
            if d % (1 << bit) == 0 and (d >> bit) & 1:
                for n in range(nblk):
                    forward(bit, d, n)
    pl.semaphore_wait(gossip.at[0], around)
    greet(gossip.at[1])
    for n in range(nblk):
        gather(1, n)
    for n in range(nblk):
        send(0, 1, n).start()
    for n in range(nblk):
        gather(0, n)
    pl.semaphore_wait(gossip.at[1], around)
    greet(gossip.at[2])
    settle(bottom_v.at[:, :, pl.ds(0, states), :], load_sem.at[2])
    convert(bottom_v, bottom_x)
    for step in range(3, outer):
        pl.semaphore_wait(gossip.at[step - 1], around)
        greet(gossip.at[step])
    settle(req_v.at[pl.ds(1, doms - 1)], req_recv.at[1])
    settle(got.at[0, 0], near_recv.at[0])
    times = [lengths_s[chosen_s[b]] for b in range(branches)]
    ones = jnp.ones((16, 3 * BLK), BF16)

    def block(n):
        tile = mine[0, n]
        for bit in range(dom_bits):
            tile = tile + got[bit, 0, n]
        turned = jnp.transpose(tile)
        w_row = tile[states + 1:states + 2, pad:2 * pad]
        l_high, l_low = split(turned[0:pad, :] * w_row)
        r_high, r_low = split(tile[:, pad:2 * pad])
        none = jnp.zeros((pad, pad), BF16)
        l_all = jnp.concatenate([
            jnp.concatenate([l_high, l_high], axis=1), jnp.concatenate([l_low, none], axis=1)
        ], axis=0)
        r_all = jnp.concatenate([
            jnp.concatenate([r_high, r_high], axis=1), jnp.concatenate([r_low, none], axis=1)
        ], axis=0)
        expo = jnp.broadcast_to(turned[pad:2 * pad, states:states + 1], (pad, BLK))
        power = expo * LOG2E
        for half in range(branches // 2):
            at = n * (branches // 2) + half
            lefts = jnp.dot(l_all, top_x[at], preferred_element_type=F32)
            rights = jnp.dot(r_all, bottom_x[at], preferred_element_type=F32)
            joint = (lefts[0:pad] + lefts[pad:2 * pad]) * (rights[0:pad] + rights[pad:2 * pad])
            for side in range(2):
                b = 2 * half + side
                decayed = joint[:, side * BLK:(side + 1) * BLK] * jnp.exp2(power * times[b])
                once = decayed * expo
                twice = once * expo
                like_v[0, b:b + 1, :] = jnp.sum(decayed, axis=0, keepdims=True)
                like_v[1, b:b + 1, :] = jnp.sum(once, axis=0, keepdims=True)
                like_v[2, b:b + 1, :] = jnp.sum(twice, axis=0, keepdims=True)
        like0 = like_v[0]
        first_d = like_v[1] / like0
        second_d = like_v[2] / like0 - first_d * first_d
        w_sites = pattern_ref[pl.ds(n, 1), :].astype(F32)
        loglik_ref[pl.ds(n, branches, stride=nblk), :] = like0
        both = jnp.concatenate([first_d, second_d], axis=0) * w_sites
        q = n % group
        for i, part in enumerate(thirds(both)):
            parts_v[n // group, q * kinds:(q + 1) * kinds, i * BLK:(i + 1) * BLK] = part
        if q == group - 1:
            sums = lax.dot_general(
                ones, parts_v[n // group], (((1,), (1,)), ((), ())), preferred_element_type=F32
            )
            pay_v[n // group:n // group + 1, :] = sums[0:1]

    for n in range(nblk):
        for bit in range(1, dom_bits):
            send(bit, 1 << bit, n).wait_recv()
        if n == min(2, nblk - 1):
            pl.semaphore_wait(gossip.at[outer - 1], around)
            for z in reversed(range(outer)):
                for x in range(inner):
                    if x or z:
                        pltpu.make_async_remote_copy(
                            src_ref=req_v,
                            dst_ref=ids_v.at[spot],
                            send_sem=ids_send.at[0],
                            recv_sem=ids_recv.at[0],
                            device_id={"site": at_site(x, z)},
                            device_id_type=MESH,
                        ).start()
            ids_v[spot] = req_v[...]
        block(n)

    peers = [(d, x, z) for d in range(doms) for x in range(inner) for z in range(outer)][1:]
    peers.sort(key=lambda peer: -(min(peer[2], outer - peer[2]) + peer[1] + peer[0] // 2))
    for d, x, z in peers:
        pltpu.make_async_remote_copy(
            src_ref=pay_v.at[pl.ds(0, rows)],
            dst_ref=pay_in.at[spot * doms + d, pl.ds(0, rows)],
            send_sem=pay_send.at[0],
            recv_sem=pay_recv.at[0],
            device_id={"dom": me ^ d, "site": at_site(x, z)},
            device_id_type=MESH,
        ).start()
    pay_in[spot * doms, 0:rows] = pay_v[0:rows]

    weights = pattern_ref[...].astype(F32)
    for b in range(branches):
        lines = pl.ds(b * nblk, nblk)
        loglik_ref[lines, :] = weights * jnp.log(loglik_ref[lines, :])
    settle(ids_v.at[pl.ds(1, sites - 1)], ids_recv.at[0])
    ids = ids_v[...].reshape(sites * doms, BLK)
    lane = lax.broadcasted_iota(jnp.int32, (sites * doms, BLK), 1)
    for n in range(nblk):
        hit = jnp.logical_and(ids[:, n:n + 1] - me * owned == lane, lane < owned)
        hit = jnp.logical_or(hit, lane == owned)
        start = (n // group) * sites * doms
        hot_v[n % group, start:start + sites * doms, :] = jnp.where(hit, 1.0, 0.0).astype(BF16)
    row = lax.broadcasted_iota(jnp.int32, (branches, BLK), 0)
    old = jnp.zeros((branches, BLK), F32)
    for b in range(branches):
        old = jnp.where(row == b, times[b], old)
    old_v[...] = old
    tree = new_ref.shape[1]
    place = lax.broadcasted_iota(jnp.int32, (1, tree), 1)
    kept = row_v[...]
    for b in range(branches):
        here = place == chosen_s[b]
        pick_v[b:b + 1, :] = jnp.where(here, 1.0, 0.0)
        kept = jnp.where(here, 0.0, kept)
    row_v[...] = kept

    settle(pay_in.at[pl.ds(1, sites * doms - 1), pl.ds(0, rows)], pay_recv.at[0])
    lines = jnp.concatenate([pay_in[:, h, :] for h in range(rows)], axis=0)
    flipped = jnp.transpose(lines)
    stacked = jnp.zeros((3 * kinds, BLK), F32)
    for q in range(group):
        third = thirds(flipped[q * kinds:(q + 1) * kinds, :])
        stacked = stacked + jnp.dot(
            jnp.concatenate(third, axis=0), hot_v[q], preferred_element_type=F32
        )
    total = stacked[0:kinds] + stacked[kinds:2 * kinds] + stacked[2 * kinds:3 * kinds]
    share_ref[...] = total[:, 0:owned]
    sums = total[:, owned:owned + 1]
    value = (old_v[...] - sums[0:branches] / sums[branches:kinds])[:, 0:1]
    chosen = jnp.where(pick_v[...] > 0.0, value, 0.0)
    new_ref[...] = row_v[...] + jnp.sum(chosen, axis=0, keepdims=True)

    for kind in range(2):
        settle(req_v.at[pl.ds(1, doms - 1)], req_send.at[kind])
    settle(ids_v.at[pl.ds(1, sites - 1)], ids_send.at[0])
    settle(pay_in.at[pl.ds(1, sites * doms - 1), pl.ds(0, rows)], pay_send.at[0])
    for d in range(1, doms):
        settle(mine.at[d], tab_send.at[d])


def store(loglik_v, share_v, new_v, loglik_ref, share_ref, new_ref, sem):
    copies = [
        pltpu.make_async_copy(source, dest, sem.at[i])
        for i, (source, dest) in enumerate((
            (new_v, new_ref), (share_v, share_ref), (loglik_v, loglik_ref)
        ))
    ]
    for copy in copies:
        copy.start()
    for copy in copies:
        copy.wait()


def on_device(
    top_partial,
    bottom_partial,
    left_vectors,
    right_vectors,
    decay_rates,
    state_weights,
    part_rates,
    branch_lengths,
    pattern_weights,
    block_partition,
    chosen_branches,
):
    doms = lax.axis_size("dom")
    sites = lax.axis_size("site")
    branches, states, _, sites_here = top_partial.shape
    nblk = sites_here // BLK
    owned = left_vectors.shape[0]
    tree = branch_lengths.shape[0]
    pad = round_up(states + 2, 64)
    dom_bits = doms.bit_length() - 1
    inner = 2 if sites % 2 == 0 else 1
    outer = sites // inner
    held = round_up(owned, 8) + 8
    kinds = 2 * branches
    group = BLK // kinds
    rows = nblk // group
    cfg = (doms, sites, inner, branches, states, nblk, owned, pad, group)
    hbm = pl.BlockSpec(memory_space=pltpu.HBM)
    vmem = pl.BlockSpec(memory_space=pltpu.VMEM)
    tile = (pad, 2 * pad)
    dma = pltpu.SemaphoreType.DMA
    pattern = pattern_weights.reshape(nblk, BLK)
    loglik, share, new = pl.pallas_call(
        functools.partial(body, cfg),
        out_shape=(
            pltpu.VMEM((branches * nblk, BLK), F32),
            pltpu.VMEM((kinds, owned), F32),
            pltpu.VMEM((1, tree), F32),
        ),
        in_specs=[hbm] * 12,
        out_specs=(vmem, vmem, vmem),
        scratch_shapes=[
            pltpu.VMEM((nblk, branches, pad, BLK), F32),
            pltpu.VMEM((nblk, branches, pad, BLK), F32),
            pltpu.VMEM((2, states, held, states), F32),
            pltpu.VMEM((doms, 1, BLK), jnp.int32),
            pltpu.SMEM((doms, 1, BLK), jnp.int32),
            pltpu.VMEM((doms, nblk) + tile, F32),
            pltpu.VMEM((doms, nblk) + tile, F32),
            pltpu.VMEM((dom_bits, doms, nblk) + tile, F32),
            pltpu.VMEM((nblk * branches // 2, 2 * pad, 2 * BLK), BF16),
            pltpu.VMEM((nblk * branches // 2, 2 * pad, 2 * BLK), BF16),
            pltpu.VMEM((3, branches, BLK), F32),
            pltpu.VMEM((rows, group * kinds, 3 * BLK), BF16),
            pltpu.VMEM((round_up(rows, 8), BLK), F32),
            pltpu.VMEM((sites * doms, round_up(rows, 8), BLK), F32),
            pltpu.VMEM((sites, doms, 1, BLK), jnp.int32),
            pltpu.VMEM((group, rows * sites * doms, BLK), BF16),
            pltpu.VMEM((branches, BLK), F32),
            pltpu.VMEM((branches, tree), F32),
            pltpu.VMEM((1, tree), F32),
            pltpu.VMEM((2, owned, states), F32),
            pltpu.SMEM((owned,), F32),
            pltpu.SMEM((tree,), F32),
            pltpu.SMEM((branches,), jnp.int32),
            pltpu.VMEM((nblk, BLK), jnp.int32),
            pltpu.SMEM((1, nblk), jnp.int32),
            pltpu.VMEM((1, nblk), jnp.int32),
            dma((4,)),
            dma((7,)),
            pltpu.SemaphoreType.REGULAR((outer,)),
            dma((2,)),
            dma((2,)),
            dma((doms,)),
            dma((1,)),
            dma((doms, nblk)),
            dma((dom_bits, nblk)),
            dma((1,)),
            dma((1,)),
            dma((1,)),
            dma((1,)),
        ],
        compiler_params=pltpu.CompilerParams(
            collective_id=0, has_side_effects=True, vmem_limit_bytes=56 * 1024 * 1024
        ),
    )(
        top_partial.reshape(branches, states, nblk, BLK),
        bottom_partial.reshape(branches, states, nblk, BLK),
        jnp.swapaxes(left_vectors, 0, 1),
        jnp.swapaxes(right_vectors, 0, 1),
        decay_rates,
        state_weights,
        part_rates,
        branch_lengths,
        chosen_branches,
        pattern,
        block_partition,
        branch_lengths.reshape(1, tree),
    )
    loglik, share, new = pl.pallas_call(
        store,
        out_shape=(
            jax.ShapeDtypeStruct((branches * nblk, BLK), F32),
            jax.ShapeDtypeStruct((kinds, owned), F32),
            jax.ShapeDtypeStruct((1, tree), F32),
        ),
        in_specs=[vmem] * 3,
        out_specs=[hbm] * 3,
        scratch_shapes=[dma((3,))],
        compiler_params=pltpu.CompilerParams(vmem_limit_bytes=1024 * 1024),
    )(loglik, share, new)
    return (
        loglik.reshape(branches, 1, sites_here),
        share.reshape(2, branches, owned),
        new.reshape(tree),
    )


def solution(mesh):
    return jax.shard_map(
        on_device,
        mesh=mesh,
        in_specs=(
            P(None, None, "dom", "site"),
            P(None, None, "dom", "site"),
            P("dom", None, None),
            P("dom", None, None),
            P("dom", None),
            P("dom", None),
            P("dom"),
            P(),
            P("dom", "site"),
            P("dom", "site"),
            P(),
        ),
        out_specs=(P(None, "dom", "site"), P(None, None, "dom"), P()),
        check_vma=False,
    )
```

```python
import functools

import jax
import jax.numpy as jnp
from jax import lax
from jax.experimental import pallas as pl
from jax.experimental.pallas import tpu as pltpu
from jax.sharding import PartitionSpec as P

BLK = 128
MESH = pl.DeviceIdType.MESH
F32 = jnp.float32
LOG2E = 1.4426950408889634
BF16 = jnp.bfloat16


def round_up(value, unit):
    return (value + unit - 1) // unit * unit


def split(value):
    high = value.astype(BF16)
    return high, (value - high.astype(F32)).astype(BF16)


def thirds(value):
    high = value.astype(BF16)
    rest = value - high.astype(F32)
    middle = rest.astype(BF16)
    return high, middle, (rest - middle.astype(F32)).astype(BF16)


def settle(ref, sem):
    pltpu.make_async_copy(ref, ref, sem).wait()


def body(
    cfg,
    top_hbm, bottom_hbm, left_hbm, right_hbm,
    decay_hbm, weight_hbm, rate_hbm, lengths_hbm, chosen_hbm,
    pattern_hbm, blocks_hbm, row_hbm,
    loglik_ref, share_ref, new_ref,
    top_v, bottom_v, tables_v, req_v, req_s, mine, passed, got, lone,
    top_x, bottom_x, like_v, parts_v, pay_v, pay_in, ids_v, hot_v, old_v, pick_v, row_v,
    modes_v, rate_s, lengths_s, chosen_s, pattern_ref, blocks_s, blocks_ref,
    load_sem, small_sem, gossip, req_send, req_recv, tab_send, lone_send, near_recv, pass_recv, far_recv,
    ids_send, ids_recv, pay_send, pay_recv,
):
    doms, sites, inner, branches, states, nblk, owned, pad, group = cfg
    me = lax.axis_index("dom")
    spot = lax.axis_index("site")
    dom_bits = doms.bit_length() - 1
    outer = sites // inner
    near, far = lax.rem(spot, inner), spot // inner
    kinds = 2 * branches
    rows = nblk // group
    slot = round_up(rows, 8)
    sent = states + 1
    early = nblk // 2

    def at_site(x, z):
        return lax.rem(far + z, outer) * inner + lax.rem(near + x, inner)

    def greet(sem):
        @pl.when(far > 0)
        def _():
            pl.semaphore_signal(
                sem, inc=1, device_id={"site": spot - inner}, device_id_type=MESH
            )

        @pl.when(far < outer - 1)
        def _():
            pl.semaphore_signal(
                sem, inc=1, device_id={"site": spot + inner}, device_id_type=MESH
            )

        for x in range(1, inner):
            pl.semaphore_signal(
                sem, inc=1, device_id={"site": at_site(x, 0)}, device_id_type=MESH
            )
        for d in reversed(range(1, doms)):
            pl.semaphore_signal(sem, inc=1, device_id={"dom": me ^ d}, device_id_type=MESH)

    odd = lax.rem(me, 2) == 1
    around = (
        doms - 1 + inner - 1 + jnp.where(far > 0, 1, 0) + jnp.where(far < outer - 1, 1, 0)
    )

    tables = [
        pltpu.make_async_copy(source, tables_v.at[pl.ds(i * states, states), pl.ds(0, owned), :], load_sem.at[0])
        for i, source in enumerate((left_hbm, right_hbm))
    ]
    tops = [
        pltpu.make_async_copy(
            top_hbm.at[:, :, n, :],
            top_v.at[n, :, pl.ds(0, states), :],
            load_sem.at[1 if n < early else 4],
        )
        for n in range(nblk)
    ]
    bottoms = [
        pltpu.make_async_copy(
            bottom_hbm.at[:, :, n, :], bottom_v.at[n, :, pl.ds(0, states), :], load_sem.at[2]
        )
        for n in range(nblk)
    ]
    modes = [
        pltpu.make_async_copy(source, modes_v.at[i], load_sem.at[3])
        for i, source in enumerate((decay_hbm, weight_hbm))
    ]
    small = [
        pltpu.make_async_copy(source, dest, small_sem.at[i])
        for i, (source, dest) in enumerate((
            (blocks_hbm, blocks_ref),
            (rate_hbm, rate_s),
            (blocks_hbm, blocks_s),
            (lengths_hbm, lengths_s),
            (chosen_hbm, chosen_s),
            (pattern_hbm, pattern_ref),
            (row_hbm, row_v),
        ))
    ]

    small[0].start()
    barrier = pltpu.get_barrier_semaphore()
    greet(barrier)
    for load in modes + tables + small[1:]:
        load.start()
    req_v[0] = jnp.zeros((1, BLK), jnp.int32)
    for side in (top_v, bottom_v):
        for n in range(nblk):
            side[n, :, states:pad, :] = jnp.zeros((branches, pad - states, BLK), F32)
    for bit in range(dom_bits):
        for d in range(0, doms, 2 << bit):
            for n in range(nblk):
                got[bit, d, n, sent:pad, :] = jnp.zeros((pad - sent, 2 * pad), F32)
    lone[...] = jnp.zeros(lone.shape, F32)
    for bit in range(1, dom_bits):
        got[bit, 0, 0] = jnp.zeros((pad, 2 * pad), F32)
    for d in range(0, doms):
        mine[d, :, sent:pad, :] = jnp.zeros((nblk, pad - sent, 2 * pad), F32)

    small[0].wait()
    req_v[0, 0:1, 0:nblk] = blocks_ref[...]
    for load in tops:
        load.start()
    pl.semaphore_wait(barrier, around)

    for kind, dest in enumerate((req_s, req_v)):
        for delta in reversed(range(1, doms)):
            pltpu.make_async_remote_copy(
                src_ref=req_v.at[0],
                dst_ref=dest.at[delta],
                send_sem=req_send.at[kind],
                recv_sem=req_recv.at[kind],
                device_id={"dom": me ^ delta},
                device_id_type=MESH,
            ).start()
    greet(gossip.at[0])
    for load in bottoms:
        load.start()

    def convert(source, dest, first, last):
        def step(n, carry):
            for b in range(branches):
                high, low = split(source[n, b])
                at = n * (branches // 2) + b // 2
                lanes = (b % 2) * BLK
                dest[at, 0:pad, lanes:lanes + BLK] = high
                dest[at, pad:2 * pad, lanes:lanes + BLK] = low
            return carry

        lax.fori_loop(first, last, step, 0)

    settle(top_v.at[pl.ds(0, early), :, pl.ds(0, states), :], load_sem.at[1])
    convert(top_v, top_x, 0, early)
    settle(modes_v, load_sem.at[3])
    settle(tables_v.at[:, pl.ds(0, owned), :], load_sem.at[0])
    for load in small[1:]:
        load.wait()
    settle(req_s.at[pl.ds(1, doms - 1)], req_recv.at[0])

    held = tables_v.shape[1]
    flat = tables_v.reshape(2 * states * held, states)

    def pick(delta, n):
        wanted = blocks_s[0, n] if delta == 0 else req_s[delta, 0, n]
        relative = wanted - me * owned
        inside = jnp.logical_and(relative >= 0, relative < owned)
        keep = jnp.where(inside, 1.0, 0.0).astype(F32)
        p = jnp.clip(relative, 0, owned - 1)
        left = jnp.concatenate(
            [flat[pl.ds(p, states, stride=held), :], modes_v[1, pl.ds(p, 1), :]], axis=0
        )
        right = jnp.concatenate(
            [flat[pl.ds(states * held + p, states, stride=held), :], modes_v[0, pl.ds(p, 1), :] * -rate_s[p]], axis=0
        )
        gap = jnp.zeros((sent, pad - states), F32)
        return jnp.concatenate([left * keep, gap, right * keep, gap], axis=1)

    def gather(delta, wanted, after=None):
        ready = pick(delta, wanted[0])
        for i, n in enumerate(wanted):
            coming = pick(delta, wanted[i + 1]) if i + 1 < len(wanted) else None
            mine[delta, n, 0:sent, :] = ready
            if after is not None:
                after(delta, n)
            ready = coming

    def send(bit, d, n):
        to = d ^ (1 << bit)
        if bit == 0:
            arrived = near_recv.at[0] if to == 0 else pass_recv.at[to // 2 - 1, n]
        else:
            arrived = far_recv.at[bit - 1, n] if to == 0 else pass_recv.at[to // 2 - 1, n]
        return pltpu.make_async_remote_copy(
            src_ref=(mine if bit == 0 else passed).at[d, n, pl.ds(0, sent)],
            dst_ref=got.at[bit, to, n, pl.ds(0, sent)],
            send_sem=tab_send.at[d - 1] if n or d == 1 else lone_send.at[1],
            recv_sem=arrived,
            device_id={"dom": me ^ (1 << bit)},
            device_id_type=MESH,
        )

    def straight(d, n):
        pltpu.make_async_remote_copy(
            src_ref=mine.at[d, n, pl.ds(0, sent)],
            dst_ref=lone.at[d, pl.ds(0, sent)],
            send_sem=lone_send.at[0],
            recv_sem=near_recv.at[1],
            device_id={"dom": me ^ d},
            device_id_type=MESH,
        ).start()

    def forward(bit, d, n):
        total = mine[d, n, 0:sent, :]
        for earlier in range(bit):
            send(earlier, d | (1 << earlier), n).wait_recv()
            total = total + got[earlier, d, n, 0:sent, :]
        passed[d, n, 0:sent, :] = total
        send(bit, d, n).start()

    rest = list(range(1, nblk))
    for d in reversed(range(2, doms)):
        gather(d, [0])

    @pl.when(odd)
    def _():
        for d in range(2, doms):
            if d & 1:
                send(0, d, 0).start()
            else:
                straight(d, 0)

    @pl.when(jnp.logical_not(odd))
    def _():
        for d in range(2, doms):
            if d & 1:
                straight(d, 0)

    for d in reversed(range(2, doms)):
        if d & 1:
            gather(d, rest, lambda d, n: send(0, d, n).start())
    for d in reversed(range(2, doms)):
        if not d & 1:
            gather(d, rest)
    for bit in range(1, dom_bits):
        for d in reversed(range(doms)):
            if d % (1 << bit) == 0 and (d >> bit) & 1:
                pl.when(jnp.logical_not(odd))(functools.partial(forward, bit, d, 0))
                for n in rest:
                    forward(bit, d, n)
    pl.semaphore_wait(gossip.at[0], around)
    greet(gossip.at[1])
    gather(1, [0] + rest)
    for n in [0] + rest:
        send(0, 1, n).start()
    gather(0, [0] + rest)
    settle(top_v.at[pl.ds(early, nblk - early), :, pl.ds(0, states), :], load_sem.at[4])
    convert(top_v, top_x, early, nblk)
    settle(bottom_v.at[:, :, pl.ds(0, states), :], load_sem.at[2])
    convert(bottom_v, bottom_x, 0, nblk)
    settle(req_v.at[pl.ds(1, doms - 1)], req_recv.at[1])
    times = [lengths_s[chosen_s[b]] for b in range(branches)]
    for h in range(rows):
        parts_v[h, 0:2 * kinds, :] = jnp.zeros((2 * kinds, 2 * BLK), BF16)
    ones = jnp.ones((16, 2 * BLK), BF16)

    def block(n):
        tile = mine[0, n]
        for bit in range(dom_bits):
            tile = tile + got[bit, 0, n]
        if n == 0:
            for d in range(2, doms):
                tile = tile + lone[d]
        turned = jnp.transpose(tile)
        w_row = tile[states:states + 1, 0:pad]
        l_high, l_low = split(turned[0:pad, :] * w_row)
        r_high, r_low = split(tile[:, pad:2 * pad])
        l_all = jnp.concatenate([l_high, l_high, l_low], axis=1)
        r_all = jnp.concatenate([r_high, r_high, r_low], axis=1)
        expo = jnp.broadcast_to(turned[pad:2 * pad, states:states + 1], (pad, BLK))
        power = expo * LOG2E
        for half in range(branches // 2):
            at = n * (branches // 2) + half
            t_x = top_x[at]
            b_x = bottom_x[at]
            lefts = jnp.dot(
                l_all, jnp.concatenate([t_x, t_x[0:pad]], axis=0), preferred_element_type=F32
            )
            rights = jnp.dot(
                r_all, jnp.concatenate([b_x, b_x[0:pad]], axis=0), preferred_element_type=F32
            )
            joint = lefts * rights
            for side in range(2):
                b = 2 * half + side
                decayed = joint[:, side * BLK:(side + 1) * BLK] * jnp.exp2(power * times[b])
                once = decayed * expo
                twice = once * expo
                like_v[n % 2, 0, b:b + 1, :] = jnp.sum(decayed, axis=0, keepdims=True)
                like_v[n % 2, 1, b:b + 1, :] = jnp.sum(once, axis=0, keepdims=True)
                like_v[n % 2, 2, b:b + 1, :] = jnp.sum(twice, axis=0, keepdims=True)
        like0 = like_v[n % 2, 0]
        first_d = like_v[n % 2, 1] / like0
        second_d = like_v[n % 2, 2] / like0 - first_d * first_d
        w_sites = pattern_ref[pl.ds(n, 1), :].astype(F32)
        loglik_ref[pl.ds(n, branches, stride=nblk), :] = like0
        both = jnp.concatenate([first_d, second_d], axis=0) * w_sites
        q = group - 1 - n % group
        for i, part in enumerate(split(both)):
            parts_v[n // group, q * kinds:(q + 1) * kinds, i * BLK:(i + 1) * BLK] = part

    def sums_of(h, count):
        return lax.dot_general(
            ones,
            parts_v[h, 0:count * kinds],
            (((1,), (1,)), ((), ())),
            preferred_element_type=F32,
        )[0:1]

    def arrive(n):
        for bit in range(1, dom_bits):
            send(bit, 1 << bit, n).wait_recv()

    @pl.when(odd)
    def _():
        settle(lone.at[pl.ds(2, doms - 2), pl.ds(0, sent)], near_recv.at[1])

    pl.when(jnp.logical_not(odd))(functools.partial(arrive, 0))
    alone = nblk // 2
    pl.semaphore_wait(gossip.at[1], around)
    greet(gossip.at[2])
    for n in range(0, alone, 2):
        if n:
            arrive(n)
        else:
            settle(got.at[0, 0, :, pl.ds(0, sent)], near_recv.at[0])
        arrive(n + 1)
        block(n)
        block(n + 1)
        if n == 0:
            for step in range(3, outer):
                pl.semaphore_wait(gossip.at[step - 1], around)
                greet(gossip.at[step])
        if n == 2:
            pl.semaphore_wait(gossip.at[outer - 1], around)
            for z in reversed(range(outer)):
                for x in range(inner):
                    if x or z:
                        pltpu.make_async_remote_copy(
                            src_ref=req_v,
                            dst_ref=ids_v.at[spot],
                            send_sem=ids_send.at[0],
                            recv_sem=ids_recv.at[0],
                            device_id={"site": at_site(x, z)},
                            device_id_type=MESH,
                        ).start()
            ids_v[spot] = req_v[...]

    for n in range(alone, nblk):
        arrive(n)
        if n == nblk - 2:
            for h in range(rows):
                pay_v[h:h + 1, :] = sums_of(h, group)
        block(n)
    late = min(2, group) * kinds
    pay_v[rows - 1:rows, 0:late] = sums_of(rows - 1, min(2, group))[:, 0:late]

    peers = [(d, x, z) for d in range(doms) for x in range(inner) for z in range(outer)][1:]
    peers.sort(key=lambda peer: -(min(peer[2], outer - peer[2]) + peer[1] + peer[0] // 2))
    for d, x, z in peers:
        pltpu.make_async_remote_copy(
            src_ref=pay_v.at[pl.ds(0, rows)],
            dst_ref=pay_in.at[pl.ds(pl.multiple_of((spot * doms + d) * slot, slot), rows)],
            send_sem=pay_send.at[0],
            recv_sem=pay_recv.at[0],
            device_id={"dom": me ^ d, "site": at_site(x, z)},
            device_id_type=MESH,
        ).start()
    pay_in[pl.ds(pl.multiple_of(spot * doms * slot, slot), rows), :] = pay_v[0:rows]

    weights = pattern_ref[...].astype(F32)
    for b in range(branches):
        lines = pl.ds(b * nblk, nblk)
        loglik_ref[lines, :] = weights * jnp.log(loglik_ref[lines, :])
    settle(ids_v.at[pl.ds(1, sites - 1)], ids_recv.at[0])
    ids = ids_v[...].reshape(sites * doms, BLK)
    lane = lax.broadcasted_iota(jnp.int32, (sites * doms, BLK), 1)
    for n in range(nblk):
        hit = jnp.logical_and(ids[:, n:n + 1] - me * owned == lane, lane < owned)
        start = (n // group) * sites * doms
        hot_v[group - 1 - n % group, start:start + sites * doms, 0:BLK] = (
            jnp.where(hit, 1.0, 0.0).astype(BF16)
        )
    hot_v[:, :, BLK:2 * BLK] = jnp.ones((group, rows * sites * doms, BLK), BF16)
    row = lax.broadcasted_iota(jnp.int32, (branches, BLK), 0)
    old = jnp.zeros((branches, BLK), F32)
    for b in range(branches):
        old = jnp.where(row == b, times[b], old)
    old_v[...] = old
    tree = new_ref.shape[1]
    place = lax.broadcasted_iota(jnp.int32, (1, tree), 1)
    kept = row_v[...]
    for b in range(branches):
        here = place == chosen_s[b]
        pick_v[b:b + 1, :] = jnp.where(here, 1.0, 0.0)
        kept = jnp.where(here, 0.0, kept)
    row_v[...] = kept

    settle(pay_in.at[pl.ds(0, (sites * doms - 1) * rows)], pay_recv.at[0])
    lines = jnp.concatenate([pay_in[pl.ds(h, sites * doms, stride=slot), :] for h in range(rows)], axis=0)
    flipped = jnp.transpose(lines)
    stacked = jnp.zeros((3 * kinds, 2 * BLK), F32)
    for q in range(group):
        third = thirds(flipped[q * kinds:(q + 1) * kinds, :])
        stacked = stacked + jnp.dot(
            jnp.concatenate(third, axis=0), hot_v[q], preferred_element_type=F32
        )
    total = stacked[0:kinds] + stacked[kinds:2 * kinds] + stacked[2 * kinds:3 * kinds]
    share_ref[...] = total[:, 0:owned]
    sums = total[:, BLK:2 * BLK]
    value = old_v[...] - sums[0:branches] / sums[branches:kinds]
    for start in range(0, tree, BLK):
        width = min(BLK, tree - start)
        lanes = slice(start, start + width)
        chosen = jnp.where(pick_v[:, lanes] > 0.0, value[:, 0:width], 0.0)
        new_ref[:, lanes] = row_v[:, lanes] + jnp.sum(chosen, axis=0, keepdims=True)

    for kind in range(2):
        settle(req_v.at[pl.ds(1, doms - 1)], req_send.at[kind])
    settle(ids_v.at[pl.ds(1, sites - 1)], ids_send.at[0])
    settle(pay_in.at[pl.ds(0, (sites * doms - 1) * rows)], pay_send.at[0])
    for i in range(2):
        settle(lone.at[pl.ds(2, doms // 2 - 1), pl.ds(0, sent)], lone_send.at[i])
    for d in range(1, doms):
        start = 0 if d == 1 else 1
        settle(mine.at[d, pl.ds(start, nblk - start), pl.ds(0, sent)], tab_send.at[d - 1])


def store(loglik_v, share_v, new_v, loglik_ref, share_ref, new_ref, sem):
    copies = [
        pltpu.make_async_copy(source, dest, sem.at[i])
        for i, (source, dest) in enumerate((
            (new_v, new_ref), (share_v, share_ref), (loglik_v, loglik_ref)
        ))
    ]
    for copy in copies:
        copy.start()
    for copy in copies:
        copy.wait()


def on_device(
    top_partial,
    bottom_partial,
    left_vectors,
    right_vectors,
    decay_rates,
    state_weights,
    part_rates,
    branch_lengths,
    pattern_weights,
    block_partition,
    chosen_branches,
):
    doms = lax.axis_size("dom")
    sites = lax.axis_size("site")
    branches, states, _, sites_here = top_partial.shape
    nblk = sites_here // BLK
    owned = left_vectors.shape[0]
    tree = branch_lengths.shape[0]
    pad = round_up(states + 2, 64)
    dom_bits = doms.bit_length() - 1
    inner = 2 if sites % 2 == 0 else 1
    outer = sites // inner
    held = round_up(owned, 8) + 8
    kinds = 2 * branches
    group = BLK // kinds
    rows = nblk // group
    cfg = (doms, sites, inner, branches, states, nblk, owned, pad, group)
    hbm = pl.BlockSpec(memory_space=pltpu.HBM)
    vmem = pl.BlockSpec(memory_space=pltpu.VMEM)
    tile = (pad, 2 * pad)
    dma = pltpu.SemaphoreType.DMA
    pattern = pattern_weights.reshape(nblk, BLK)
    loglik, share, new = pl.pallas_call(
        functools.partial(body, cfg),
        out_shape=(
            pltpu.VMEM((branches * nblk, BLK), F32),
            pltpu.VMEM((kinds, owned), F32),
            pltpu.VMEM((1, tree), F32),
        ),
        in_specs=[hbm] * 12,
        out_specs=(vmem, vmem, vmem),
        scratch_shapes=[
            pltpu.VMEM((nblk, branches, pad, BLK), F32),
            pltpu.VMEM((nblk, branches, pad, BLK), F32),
            pltpu.VMEM((2 * states, held, states), F32),
            pltpu.VMEM((doms, 1, BLK), jnp.int32),
            pltpu.SMEM((doms, 1, BLK), jnp.int32),
            pltpu.VMEM((doms, nblk) + tile, F32),
            pltpu.VMEM((doms, nblk) + tile, F32),
            pltpu.VMEM((dom_bits, doms, nblk) + tile, F32),
            pltpu.VMEM((doms,) + tile, F32),
            pltpu.VMEM((nblk * branches // 2, 2 * pad, 2 * BLK), BF16),
            pltpu.VMEM((nblk * branches // 2, 2 * pad, 2 * BLK), BF16),
            pltpu.VMEM((2, 3, branches, BLK), F32),
            pltpu.VMEM((rows, group * kinds, 2 * BLK), BF16),
            pltpu.VMEM((round_up(rows, 8), BLK), F32),
            pltpu.VMEM((sites * doms * round_up(rows, 8), BLK), F32),
            pltpu.VMEM((sites, doms, 1, BLK), jnp.int32),
            pltpu.VMEM((group, rows * sites * doms, 2 * BLK), BF16),
            pltpu.VMEM((branches, BLK), F32),
            pltpu.VMEM((branches, tree), F32),
            pltpu.VMEM((1, tree), F32),
            pltpu.VMEM((2, owned, states), F32),
            pltpu.SMEM((owned,), F32),
            pltpu.SMEM((tree,), F32),
            pltpu.SMEM((branches,), jnp.int32),
            pltpu.VMEM((nblk, BLK), jnp.int32),
            pltpu.SMEM((1, nblk), jnp.int32),
            pltpu.VMEM((1, nblk), jnp.int32),
            dma((5,)),
            dma((7,)),
            pltpu.SemaphoreType.REGULAR((outer,)),
            dma((2,)),
            dma((2,)),
            dma((doms - 1,)),
            dma((2,)),
            dma((2,)),
            dma((doms // 2 - 1, nblk)),
            dma((dom_bits - 1, nblk)),
            dma((1,)),
            dma((1,)),
            dma((1,)),
            dma((1,)),
        ],
        compiler_params=pltpu.CompilerParams(
            collective_id=0, has_side_effects=True, vmem_limit_bytes=56 * 1024 * 1024
        ),
    )(
        top_partial.reshape(branches, states, nblk, BLK),
        bottom_partial.reshape(branches, states, nblk, BLK),
        jnp.swapaxes(left_vectors, 0, 1),
        jnp.swapaxes(right_vectors, 0, 1),
        decay_rates,
        state_weights,
        part_rates,
        branch_lengths,
        chosen_branches,
        pattern,
        block_partition,
        branch_lengths.reshape(1, tree),
    )
    loglik, share, new = pl.pallas_call(
        store,
        out_shape=(
            jax.ShapeDtypeStruct((branches * nblk, BLK), F32),
            jax.ShapeDtypeStruct((kinds, owned), F32),
            jax.ShapeDtypeStruct((1, tree), F32),
        ),
        in_specs=[vmem] * 3,
        out_specs=[hbm] * 3,
        scratch_shapes=[dma((3,))],
        compiler_params=pltpu.CompilerParams(vmem_limit_bytes=1024 * 1024),
    )(loglik, share, new)
    return (
        loglik.reshape(branches, 1, sites_here),
        share.reshape(2, branches, owned),
        new.reshape(tree),
    )


def solution(mesh):
    return jax.shard_map(
        on_device,
        mesh=mesh,
        in_specs=(
            P(None, None, "dom", "site"),
            P(None, None, "dom", "site"),
            P("dom", None, None),
            P("dom", None, None),
            P("dom", None),
            P("dom", None),
            P("dom"),
            P(),
            P("dom", "site"),
            P("dom", "site"),
            P(),
        ),
        out_specs=(P(None, "dom", "site"), P(None, None, "dom"), P()),
        check_vma=False,
    )
```

```python
import functools

import jax
import jax.numpy as jnp
from jax import lax
from jax.experimental import pallas as pl
from jax.experimental.pallas import tpu as pltpu
from jax.sharding import PartitionSpec as P

BLK = 128
MESH = pl.DeviceIdType.MESH
F32 = jnp.float32
LOG2E = 1.4426950408889634
BF16 = jnp.bfloat16


def round_up(value, unit):
    return (value + unit - 1) // unit * unit


def split(value):
    high = value.astype(BF16)
    return high, (value - high.astype(F32)).astype(BF16)


def thirds(value):
    high = value.astype(BF16)
    rest = value - high.astype(F32)
    middle = rest.astype(BF16)
    return high, middle, (rest - middle.astype(F32)).astype(BF16)


def settle(ref, sem):
    pltpu.make_async_copy(ref, ref, sem).wait()


def body(
    cfg,
    top_hbm, bottom_hbm, left_hbm, right_hbm,
    decay_hbm, weight_hbm, rate_hbm, lengths_hbm, chosen_hbm,
    pattern_hbm, blocks_hbm, row_hbm,
    loglik_ref, share_ref, new_ref,
    top_v, bottom_v, tables_v, req_v, req_s, mine, passed, near_v, far_v, lone,
    top_x, bottom_x, like_v, parts_v, pay_v, pay_in, ids_v, hot_v, old_v, pick_v, row_v,
    modes_v, rate_s, lengths_s, chosen_s, pattern_ref, blocks_s, blocks_ref,
    load_sem, small_sem, gossip, req_send, req_recv, tab_send, lone_send, near_recv, pass_recv, far_recv,
    ids_send, ids_recv, pay_send, pay_recv,
):
    doms, sites, inner, branches, states, nblk, owned, pad, group = cfg
    me = lax.axis_index("dom")
    spot = lax.axis_index("site")
    outer = sites // inner
    near, far = lax.rem(spot, inner), spot // inner
    kinds = 2 * branches
    rows = nblk // group
    slot = round_up(rows, 8)
    sent = states
    early = nblk // 2

    def at_site(x, z):
        return lax.rem(far + z, outer) * inner + lax.rem(near + x, inner)

    def greet(sem):
        @pl.when(far > 0)
        def _():
            pl.semaphore_signal(
                sem, inc=1, device_id={"site": spot - inner}, device_id_type=MESH
            )

        @pl.when(far < outer - 1)
        def _():
            pl.semaphore_signal(
                sem, inc=1, device_id={"site": spot + inner}, device_id_type=MESH
            )

        for x in range(1, inner):
            pl.semaphore_signal(
                sem, inc=1, device_id={"site": at_site(x, 0)}, device_id_type=MESH
            )
        for d in reversed(range(1, doms)):
            pl.semaphore_signal(sem, inc=1, device_id={"dom": me ^ d}, device_id_type=MESH)

    odd = lax.rem(me, 2) == 1
    around = (
        doms - 1 + inner - 1 + jnp.where(far > 0, 1, 0) + jnp.where(far < outer - 1, 1, 0)
    )

    tables = [
        pltpu.make_async_copy(source, tables_v.at[pl.ds(i * states, states), pl.ds(0, owned), :], load_sem.at[0])
        for i, source in enumerate((left_hbm, right_hbm))
    ]
    tops = [
        pltpu.make_async_copy(
            top_hbm.at[:, :, n, :],
            top_v.at[n, :, pl.ds(0, states), :],
            load_sem.at[1 if n < early else 4],
        )
        for n in range(nblk)
    ]
    bottoms = [
        pltpu.make_async_copy(
            bottom_hbm.at[:, :, n, :], bottom_v.at[n, :, pl.ds(0, states), :], load_sem.at[2]
        )
        for n in range(nblk)
    ]
    modes = [
        pltpu.make_async_copy(source, modes_v.at[i], load_sem.at[3])
        for i, source in enumerate((decay_hbm, weight_hbm))
    ]
    small = [
        pltpu.make_async_copy(source, dest, small_sem.at[i])
        for i, (source, dest) in enumerate((
            (blocks_hbm, blocks_ref),
            (rate_hbm, rate_s),
            (blocks_hbm, blocks_s),
            (lengths_hbm, lengths_s),
            (chosen_hbm, chosen_s),
            (pattern_hbm, pattern_ref),
            (row_hbm, row_v),
        ))
    ]

    small[0].start()
    barrier = pltpu.get_barrier_semaphore()
    greet(barrier)
    for load in modes + tables + small[1:]:
        load.start()
    req_v[0] = jnp.zeros((1, BLK), jnp.int32)
    for side in (top_v, bottom_v):
        for n in range(nblk):
            side[n, :, states:pad, :] = jnp.zeros((branches, pad - states, BLK), F32)
    for n in range(nblk):
        near_v[0, n, sent:pad, :] = jnp.zeros((pad - sent, 2 * pad), F32)
        for k in range(1, doms // 2):
            far_v[k, n, sent:pad, :] = jnp.zeros((pad - sent, 2 * pad), F32)
    for d in range(2, doms):
        lone[d, sent:pad, :] = jnp.zeros((pad - sent, 2 * pad), F32)
    mine[0, :, sent:pad, :] = jnp.zeros((nblk, pad - sent, 2 * pad), F32)

    small[0].wait()
    req_v[0, 0:1, 0:nblk] = blocks_ref[...]
    for load in tops:
        load.start()
    pl.semaphore_wait(barrier, around)

    for kind, dest in enumerate((req_s, req_v)):
        for delta in reversed(range(1, doms)):
            pltpu.make_async_remote_copy(
                src_ref=req_v.at[0],
                dst_ref=dest.at[delta],
                send_sem=req_send.at[kind],
                recv_sem=req_recv.at[kind],
                device_id={"dom": me ^ delta},
                device_id_type=MESH,
            ).start()
    greet(gossip.at[0])
    for load in bottoms:
        load.start()

    def convert(source, dest, first, last):
        def step(n, carry):
            for b in range(branches):
                high, low = split(source[n, b])
                at = n * (branches // 2) + b // 2
                lanes = (b % 2) * BLK
                dest[at, 0:pad, lanes:lanes + BLK] = high
                dest[at, pad:2 * pad, lanes:lanes + BLK] = low
            return carry

        lax.fori_loop(first, last, step, 0)

    settle(top_v.at[pl.ds(0, early), :, pl.ds(0, states), :], load_sem.at[1])
    convert(top_v, top_x, 0, early)
    settle(modes_v, load_sem.at[3])
    settle(tables_v.at[:, pl.ds(0, owned), :], load_sem.at[0])
    for load in small[1:]:
        load.wait()
    settle(req_s.at[pl.ds(1, doms - 1)], req_recv.at[0])

    held = tables_v.shape[1]
    flat = tables_v.reshape(2 * states * held, states)

    def pick(delta, n):
        wanted = blocks_s[0, n] if delta == 0 else req_s[delta, 0, n]
        relative = wanted - me * owned
        inside = jnp.logical_and(relative >= 0, relative < owned)
        keep = jnp.where(inside, 1.0, 0.0).astype(F32)
        p = jnp.clip(relative, 0, owned - 1)
        left = jnp.concatenate([
            flat[pl.ds(p, states, stride=held), :],
            modes_v[0, pl.ds(p, 1), :] * -rate_s[p],
            jnp.zeros((pad - states - 1, states), F32),
        ], axis=0)
        right = flat[pl.ds(states * held + p, states, stride=held), :]
        turned = jnp.transpose(
            jnp.concatenate([left, jnp.zeros((pad, 2 * pad - states), F32)], axis=1)
        )
        scale = jnp.concatenate([
            modes_v[1, pl.ds(p, 1), :] * keep,
            jnp.full((1, 1), keep),
            jnp.zeros((1, pad - states - 1), F32),
        ], axis=1)
        gap = jnp.zeros((states, pad - states), F32)
        return jnp.concatenate([turned[0:states, :] * scale, right * keep, gap], axis=1)

    def gather(wanted, after=None):
        ready = pick(*wanted[0])
        for i, (delta, n) in enumerate(wanted):
            coming = pick(*wanted[i + 1]) if i + 1 < len(wanted) else None
            mine[delta, n, 0:sent, :] = ready
            if after is not None:
                after(delta, n)
            ready = coming

    def beside(d, n):
        pltpu.make_async_remote_copy(
            src_ref=mine.at[d, n, pl.ds(0, sent)],
            dst_ref=near_v.at[d ^ 1, n, pl.ds(0, sent)],
            send_sem=tab_send.at[1 if d == 1 else 0],
            recv_sem=near_recv.at[0] if d == 1 else pass_recv.at[n - 1],
            device_id={"dom": me ^ 1},
            device_id_type=MESH,
        ).start()

    def straight(d):
        pltpu.make_async_remote_copy(
            src_ref=mine.at[d, 0, pl.ds(0, sent)],
            dst_ref=lone.at[d, pl.ds(0, sent)],
            send_sem=lone_send.at[0],
            recv_sem=near_recv.at[1],
            device_id={"dom": me ^ d},
            device_id_type=MESH,
        ).start()

    def beyond(d, n):
        passed[d, n, 0:sent, :] = mine[d, n, 0:sent, :] + near_v[d, n, 0:sent, :]
        pltpu.make_async_remote_copy(
            src_ref=passed.at[d, n, pl.ds(0, sent)],
            dst_ref=far_v.at[d // 2, n, pl.ds(0, sent)],
            send_sem=tab_send.at[0],
            recv_sem=far_recv.at[d // 2 - 1, n - 1],
            device_id={"dom": me ^ d},
            device_id_type=MESH,
        ).start()

    others = list(reversed(range(2, doms)))
    gather([(d, 0) for d in others])
    for d in others:
        straight(d)
    pairs = [(d, n) for n in range(1, nblk) for d in others]

    @pl.when(jnp.logical_not(odd))
    def _():
        gather(pairs, beside)

    @pl.when(odd)
    def _():
        gather(pairs)

    gather([(1, n) for n in range(nblk)])
    for n in range(nblk):
        beside(1, n)
    gather([(0, n) for n in range(nblk)])

    @pl.when(odd)
    def _():
        for n in range(1, nblk):
            settle(near_v.at[pl.ds(2, doms - 2), n, pl.ds(0, sent)], pass_recv.at[n - 1])
            for d in others:
                beyond(d, n)

    pl.semaphore_wait(gossip.at[0], around)
    greet(gossip.at[1])
    settle(top_v.at[pl.ds(early, nblk - early), :, pl.ds(0, states), :], load_sem.at[4])
    convert(top_v, top_x, early, nblk)
    settle(bottom_v.at[:, :, pl.ds(0, states), :], load_sem.at[2])
    convert(bottom_v, bottom_x, 0, nblk)
    settle(req_v.at[pl.ds(1, doms - 1)], req_recv.at[1])
    times = [lengths_s[chosen_s[b]] for b in range(branches)]
    for h in range(rows):
        parts_v[h, 0:2 * kinds, :] = jnp.zeros((2 * kinds, 2 * BLK), BF16)
    ones = jnp.ones((16, 2 * BLK), BF16)

    def block(n):
        tile = mine[0, n]
        tile = tile + near_v[0, n]
        if n == 0:
            for d in range(2, doms):
                tile = tile + lone[d]
        else:
            for k in range(1, doms // 2):
                tile = tile + far_v[k, n]
        l_high, l_low = split(tile[:, 0:pad])
        r_high, r_low = split(tile[:, pad:2 * pad])
        l_all = jnp.concatenate([l_high, l_high, l_low], axis=1)
        r_all = jnp.concatenate([r_high, r_high, r_low], axis=1)
        expo = jnp.broadcast_to(tile[:, states:states + 1], (pad, BLK))
        power = expo * LOG2E
        for half in range(branches // 2):
            at = n * (branches // 2) + half
            t_x = top_x[at]
            b_x = bottom_x[at]
            lefts = jnp.dot(
                l_all, jnp.concatenate([t_x, t_x[0:pad]], axis=0), preferred_element_type=F32
            )
            rights = jnp.dot(
                r_all, jnp.concatenate([b_x, b_x[0:pad]], axis=0), preferred_element_type=F32
            )
            joint = lefts * rights
            for side in range(2):
                b = 2 * half + side
                decayed = joint[:, side * BLK:(side + 1) * BLK] * jnp.exp2(power * times[b])
                once = decayed * expo
                twice = once * expo
                like_v[n % 2, 0, b:b + 1, :] = jnp.sum(decayed, axis=0, keepdims=True)
                like_v[n % 2, 1, b:b + 1, :] = jnp.sum(once, axis=0, keepdims=True)
                like_v[n % 2, 2, b:b + 1, :] = jnp.sum(twice, axis=0, keepdims=True)
        like0 = like_v[n % 2, 0]
        first_d = like_v[n % 2, 1] / like0
        second_d = like_v[n % 2, 2] / like0 - first_d * first_d
        w_sites = pattern_ref[pl.ds(n, 1), :].astype(F32)
        loglik_ref[pl.ds(n, branches, stride=nblk), :] = like0
        both = jnp.concatenate([first_d, second_d], axis=0) * w_sites
        q = group - 1 - n % group
        for i, part in enumerate(split(both)):
            parts_v[n // group, q * kinds:(q + 1) * kinds, i * BLK:(i + 1) * BLK] = part

    def sums_of(h, count):
        return lax.dot_general(
            ones,
            parts_v[h, 0:count * kinds],
            (((1,), (1,)), ((), ())),
            preferred_element_type=F32,
        )[0:1]

    def arrive(n):
        for k in range(1, doms // 2):
            settle(far_v.at[k, n, pl.ds(0, sent)], far_recv.at[k - 1, n - 1])

    settle(lone.at[pl.ds(2, doms - 2), pl.ds(0, sent)], near_recv.at[1])
    alone = nblk // 2
    pl.semaphore_wait(gossip.at[1], around)
    greet(gossip.at[2])
    for n in range(0, alone, 2):
        if n:
            arrive(n)
        else:
            settle(near_v.at[0, :, pl.ds(0, sent)], near_recv.at[0])
        arrive(n + 1)
        block(n)
        block(n + 1)
        if n == 0:
            for step in range(3, outer):
                pl.semaphore_wait(gossip.at[step - 1], around)
                greet(gossip.at[step])
        if n == 2:
            pl.semaphore_wait(gossip.at[outer - 1], around)
            for z in reversed(range(outer)):
                for x in range(inner):
                    if x or z:
                        pltpu.make_async_remote_copy(
                            src_ref=req_v,
                            dst_ref=ids_v.at[spot],
                            send_sem=ids_send.at[0],
                            recv_sem=ids_recv.at[0],
                            device_id={"site": at_site(x, z)},
                            device_id_type=MESH,
                        ).start()
            ids_v[spot] = req_v[...]

    for n in range(alone, nblk):
        arrive(n)
        if n == nblk - 2:
            for h in range(rows):
                pay_v[h:h + 1, :] = sums_of(h, group)
        block(n)
    late = min(2, group) * kinds
    pay_v[rows - 1:rows, 0:late] = sums_of(rows - 1, min(2, group))[:, 0:late]

    peers = [(d, x, z) for d in range(doms) for x in range(inner) for z in range(outer)][1:]
    peers.sort(key=lambda peer: -(max(peer[2], -peer[2] % outer) + peer[1] + peer[0] // 2))
    for d, x, z in peers:
        pltpu.make_async_remote_copy(
            src_ref=pay_v.at[pl.ds(0, rows)],
            dst_ref=pay_in.at[pl.ds(pl.multiple_of((spot * doms + d) * slot, slot), rows)],
            send_sem=pay_send.at[0],
            recv_sem=pay_recv.at[0],
            device_id={"dom": me ^ d, "site": at_site(x, z)},
            device_id_type=MESH,
        ).start()
    pay_in[pl.ds(pl.multiple_of(spot * doms * slot, slot), rows), :] = pay_v[0:rows]

    weights = pattern_ref[...].astype(F32)
    for b in range(branches):
        lines = pl.ds(b * nblk, nblk)
        loglik_ref[lines, :] = weights * jnp.log(loglik_ref[lines, :])
    settle(ids_v.at[pl.ds(1, sites - 1)], ids_recv.at[0])
    ids = ids_v[...].reshape(sites * doms, BLK)
    lane = lax.broadcasted_iota(jnp.int32, (sites * doms, BLK), 1)
    for n in range(nblk):
        hit = jnp.logical_and(ids[:, n:n + 1] - me * owned == lane, lane < owned)
        start = (n // group) * sites * doms
        hot_v[group - 1 - n % group, start:start + sites * doms, 0:BLK] = (
            jnp.where(hit, 1.0, 0.0).astype(BF16)
        )
    hot_v[:, :, BLK:2 * BLK] = jnp.ones((group, rows * sites * doms, BLK), BF16)
    row = lax.broadcasted_iota(jnp.int32, (branches, BLK), 0)
    old = jnp.zeros((branches, BLK), F32)
    for b in range(branches):
        old = jnp.where(row == b, times[b], old)
    old_v[...] = old
    tree = new_ref.shape[1]
    place = lax.broadcasted_iota(jnp.int32, (1, tree), 1)
    kept = row_v[...]
    for b in range(branches):
        here = place == chosen_s[b]
        pick_v[b:b + 1, :] = jnp.where(here, 1.0, 0.0)
        kept = jnp.where(here, 0.0, kept)
    row_v[...] = kept

    settle(pay_in.at[pl.ds(0, (sites * doms - 1) * rows)], pay_recv.at[0])
    lines = jnp.concatenate([pay_in[pl.ds(h, sites * doms, stride=slot), :] for h in range(rows)], axis=0)
    flipped = jnp.transpose(lines)
    stacked = jnp.zeros((3 * kinds, 2 * BLK), F32)
    for q in range(group):
        third = thirds(flipped[q * kinds:(q + 1) * kinds, :])
        stacked = stacked + jnp.dot(
            jnp.concatenate(third, axis=0), hot_v[q], preferred_element_type=F32
        )
    total = stacked[0:kinds] + stacked[kinds:2 * kinds] + stacked[2 * kinds:3 * kinds]
    share_ref[...] = total[:, 0:owned]
    sums = total[:, BLK:2 * BLK]
    value = old_v[...] - sums[0:branches] / sums[branches:kinds]
    for start in range(0, tree, BLK):
        width = min(BLK, tree - start)
        lanes = slice(start, start + width)
        chosen = jnp.where(pick_v[:, lanes] > 0.0, value[:, 0:width], 0.0)
        new_ref[:, lanes] = row_v[:, lanes] + jnp.sum(chosen, axis=0, keepdims=True)

    for kind in range(2):
        settle(req_v.at[pl.ds(1, doms - 1)], req_send.at[kind])
    settle(ids_v.at[pl.ds(1, sites - 1)], ids_send.at[0])
    settle(pay_in.at[pl.ds(0, (sites * doms - 1) * rows)], pay_send.at[0])
    settle(lone.at[pl.ds(2, doms - 2), pl.ds(0, sent)], lone_send.at[0])
    settle(
        mine.at[pl.ds(2, doms - 2), pl.ds(1, nblk - 1), pl.ds(0, sent)], tab_send.at[0]
    )
    settle(mine.at[1, :, pl.ds(0, sent)], tab_send.at[1])


def store(loglik_v, share_v, new_v, loglik_ref, share_ref, new_ref, sem):
    copies = [
        pltpu.make_async_copy(source, dest, sem.at[i])
        for i, (source, dest) in enumerate((
            (new_v, new_ref), (share_v, share_ref), (loglik_v, loglik_ref)
        ))
    ]
    for copy in copies:
        copy.start()
    for copy in copies:
        copy.wait()


def on_device(
    top_partial,
    bottom_partial,
    left_vectors,
    right_vectors,
    decay_rates,
    state_weights,
    part_rates,
    branch_lengths,
    pattern_weights,
    block_partition,
    chosen_branches,
):
    doms = lax.axis_size("dom")
    sites = lax.axis_size("site")
    branches, states, _, sites_here = top_partial.shape
    nblk = sites_here // BLK
    owned = left_vectors.shape[0]
    tree = branch_lengths.shape[0]
    pad = round_up(states + 2, 64)
    inner = 2 if sites % 2 == 0 else 1
    outer = sites // inner
    held = round_up(owned, 8) + 8
    kinds = 2 * branches
    group = BLK // kinds
    rows = nblk // group
    cfg = (doms, sites, inner, branches, states, nblk, owned, pad, group)
    hbm = pl.BlockSpec(memory_space=pltpu.HBM)
    vmem = pl.BlockSpec(memory_space=pltpu.VMEM)
    tile = (pad, 2 * pad)
    dma = pltpu.SemaphoreType.DMA
    pattern = pattern_weights.reshape(nblk, BLK)
    loglik, share, new = pl.pallas_call(
        functools.partial(body, cfg),
        out_shape=(
            pltpu.VMEM((branches * nblk, BLK), F32),
            pltpu.VMEM((kinds, owned), F32),
            pltpu.VMEM((1, tree), F32),
        ),
        in_specs=[hbm] * 12,
        out_specs=(vmem, vmem, vmem),
        scratch_shapes=[
            pltpu.VMEM((nblk, branches, pad, BLK), F32),
            pltpu.VMEM((nblk, branches, pad, BLK), F32),
            pltpu.VMEM((2 * states, held, states), F32),
            pltpu.VMEM((doms, 1, BLK), jnp.int32),
            pltpu.SMEM((doms, 1, BLK), jnp.int32),
            pltpu.VMEM((doms, nblk) + tile, F32),
            pltpu.VMEM((doms, nblk) + tile, F32),
            pltpu.VMEM((doms, nblk) + tile, F32),
            pltpu.VMEM((doms // 2, nblk) + tile, F32),
            pltpu.VMEM((doms,) + tile, F32),
            pltpu.VMEM((nblk * branches // 2, 2 * pad, 2 * BLK), BF16),
            pltpu.VMEM((nblk * branches // 2, 2 * pad, 2 * BLK), BF16),
            pltpu.VMEM((2, 3, branches, BLK), F32),
            pltpu.VMEM((rows, group * kinds, 2 * BLK), BF16),
            pltpu.VMEM((round_up(rows, 8), BLK), F32),
            pltpu.VMEM((sites * doms * round_up(rows, 8), BLK), F32),
            pltpu.VMEM((sites, doms, 1, BLK), jnp.int32),
            pltpu.VMEM((group, rows * sites * doms, 2 * BLK), BF16),
            pltpu.VMEM((branches, BLK), F32),
            pltpu.VMEM((branches, tree), F32),
            pltpu.VMEM((1, tree), F32),
            pltpu.VMEM((2, owned, states), F32),
            pltpu.SMEM((owned,), F32),
            pltpu.SMEM((tree,), F32),
            pltpu.SMEM((branches,), jnp.int32),
            pltpu.VMEM((nblk, BLK), jnp.int32),
            pltpu.SMEM((1, nblk), jnp.int32),
            pltpu.VMEM((1, nblk), jnp.int32),
            dma((5,)),
            dma((7,)),
            pltpu.SemaphoreType.REGULAR((outer,)),
            dma((2,)),
            dma((2,)),
            dma((2,)),
            dma((1,)),
            dma((2,)),
            dma((nblk - 1,)),
            dma((doms // 2 - 1, nblk - 1)),
            dma((1,)),
            dma((1,)),
            dma((1,)),
            dma((1,)),
        ],
        compiler_params=pltpu.CompilerParams(
            collective_id=0, has_side_effects=True, vmem_limit_bytes=56 * 1024 * 1024
        ),
    )(
        top_partial.reshape(branches, states, nblk, BLK),
        bottom_partial.reshape(branches, states, nblk, BLK),
        jnp.swapaxes(left_vectors, 0, 1),
        jnp.swapaxes(right_vectors, 0, 1),
        decay_rates,
        state_weights,
        part_rates,
        branch_lengths,
        chosen_branches,
        pattern,
        block_partition,
        branch_lengths.reshape(1, tree),
    )
    loglik, share, new = pl.pallas_call(
        store,
        out_shape=(
            jax.ShapeDtypeStruct((branches * nblk, BLK), F32),
            jax.ShapeDtypeStruct((kinds, owned), F32),
            jax.ShapeDtypeStruct((1, tree), F32),
        ),
        in_specs=[vmem] * 3,
        out_specs=[hbm] * 3,
        scratch_shapes=[dma((3,))],
        compiler_params=pltpu.CompilerParams(vmem_limit_bytes=1024 * 1024),
    )(loglik, share, new)
    return (
        loglik.reshape(branches, 1, sites_here),
        share.reshape(2, branches, owned),
        new.reshape(tree),
    )


def solution(mesh):
    return jax.shard_map(
        on_device,
        mesh=mesh,
        in_specs=(
            P(None, None, "dom", "site"),
            P(None, None, "dom", "site"),
            P("dom", None, None),
            P("dom", None, None),
            P("dom", None),
            P("dom", None),
            P("dom"),
            P(),
            P("dom", "site"),
            P("dom", "site"),
            P(),
        ),
        out_specs=(P(None, "dom", "site"), P(None, None, "dom"), P()),
        check_vma=False,
    )
```

```python
import functools

import jax
import jax.numpy as jnp
from jax import lax
from jax.experimental import pallas as pl
from jax.experimental.pallas import tpu as pltpu
from jax.sharding import PartitionSpec as P

BLK = 128
MESH = pl.DeviceIdType.MESH
F32 = jnp.float32
LOG2E = 1.4426950408889634
BF16 = jnp.bfloat16


def round_up(value, unit):
    return (value + unit - 1) // unit * unit


def split(value):
    high = value.astype(BF16)
    return high, (value - high.astype(F32)).astype(BF16)


def thirds(value):
    high = value.astype(BF16)
    rest = value - high.astype(F32)
    middle = rest.astype(BF16)
    return high, middle, (rest - middle.astype(F32)).astype(BF16)


def settle(ref, sem):
    pltpu.make_async_copy(ref, ref, sem).wait()


def body(
    cfg,
    top_hbm, bottom_hbm, left_hbm, right_hbm,
    decay_hbm, weight_hbm, rate_hbm, lengths_hbm, chosen_hbm,
    pattern_hbm, blocks_hbm, row_hbm,
    loglik_ref, share_ref, new_ref,
    top_v, bottom_v, tables_v, req_v, req_s, mine, passed, near_v, far_v, lone,
    top_x, bottom_x, like_v, parts_v, pay_v, pay_in, ids_v, hot_v, old_v, pick_v, row_v,
    modes_v, rate_s, lengths_s, chosen_s, pattern_ref, blocks_s, blocks_ref,
    load_sem, small_sem, gossip, req_send, req_recv, tab_send, lone_send, near_recv, pass_recv, far_recv,
    ids_send, ids_recv, pay_send, pay_recv,
):
    doms, sites, inner, branches, states, nblk, owned, pad, group = cfg
    me = lax.axis_index("dom")
    spot = lax.axis_index("site")
    outer = sites // inner
    near, far = lax.rem(spot, inner), spot // inner
    kinds = 2 * branches
    rows = nblk // group
    slot = round_up(rows, 8)
    sent = states
    early = nblk // 2

    def at_site(x, z):
        return lax.rem(far + z, outer) * inner + lax.rem(near + x, inner)

    def greet(sem):
        @pl.when(far > 0)
        def _():
            pl.semaphore_signal(
                sem, inc=1, device_id={"site": spot - inner}, device_id_type=MESH
            )

        @pl.when(far < outer - 1)
        def _():
            pl.semaphore_signal(
                sem, inc=1, device_id={"site": spot + inner}, device_id_type=MESH
            )

        for x in range(1, inner):
            pl.semaphore_signal(
                sem, inc=1, device_id={"site": at_site(x, 0)}, device_id_type=MESH
            )
        for d in reversed(range(1, doms)):
            pl.semaphore_signal(sem, inc=1, device_id={"dom": me ^ d}, device_id_type=MESH)

    odd = lax.rem(me, 2) == 1
    around = (
        doms - 1 + inner - 1 + jnp.where(far > 0, 1, 0) + jnp.where(far < outer - 1, 1, 0)
    )

    tables = [
        pltpu.make_async_copy(source, tables_v.at[pl.ds(i * states, states), pl.ds(0, owned), :], load_sem.at[0])
        for i, source in enumerate((left_hbm, right_hbm))
    ]
    tops = [
        pltpu.make_async_copy(
            top_hbm.at[:, :, n, :],
            top_v.at[n, :, pl.ds(0, states), :],
            load_sem.at[1 if n < early else 4],
        )
        for n in range(nblk)
    ]
    bottoms = [
        pltpu.make_async_copy(
            bottom_hbm.at[:, :, n, :], bottom_v.at[n, :, pl.ds(0, states), :], load_sem.at[2]
        )
        for n in range(nblk)
    ]
    modes = [
        pltpu.make_async_copy(source, modes_v.at[i], load_sem.at[3])
        for i, source in enumerate((decay_hbm, weight_hbm))
    ]
    small = [
        pltpu.make_async_copy(source, dest, small_sem.at[i])
        for i, (source, dest) in enumerate((
            (blocks_hbm, blocks_ref),
            (rate_hbm, rate_s),
            (blocks_hbm, blocks_s),
            (lengths_hbm, lengths_s),
            (chosen_hbm, chosen_s),
            (pattern_hbm, pattern_ref),
            (row_hbm, row_v),
        ))
    ]

    small[0].start()
    barrier = pltpu.get_barrier_semaphore()
    greet(barrier)
    for load in modes + tables + small[1:]:
        load.start()
    req_v[0] = jnp.zeros((1, BLK), jnp.int32)
    for side in (top_v, bottom_v):
        for n in range(nblk):
            side[n, :, states:pad, :] = jnp.zeros((branches, pad - states, BLK), F32)
    for n in range(nblk):
        near_v[0, n, sent:pad, :] = jnp.zeros((pad - sent, 2 * pad), F32)
        for k in range(1, doms // 2):
            far_v[k, n, sent:pad, :] = jnp.zeros((pad - sent, 2 * pad), F32)
    for d in range(2, doms):
        lone[d, sent:pad, :] = jnp.zeros((pad - sent, 2 * pad), F32)
    mine[0, :, sent:pad, :] = jnp.zeros((nblk, pad - sent, 2 * pad), F32)

    small[0].wait()
    req_v[0, 0:1, 0:nblk] = blocks_ref[...]
    for load in tops:
        load.start()
    pl.semaphore_wait(barrier, around)

    for kind, dest in enumerate((req_s, req_v)):
        for delta in reversed(range(1, doms)):
            pltpu.make_async_remote_copy(
                src_ref=req_v.at[0],
                dst_ref=dest.at[delta],
                send_sem=req_send.at[kind],
                recv_sem=req_recv.at[0 if kind else delta],
                device_id={"dom": me ^ delta},
                device_id_type=MESH,
            ).start()
    greet(gossip.at[0])
    for load in bottoms:
        load.start()

    def convert(source, dest, first, last):
        def step(n, carry):
            for b in range(branches):
                high, low = split(source[n, b])
                at = n * (branches // 2) + b // 2
                lanes = (b % 2) * BLK
                dest[at, 0:pad, lanes:lanes + BLK] = high
                dest[at, pad:2 * pad, lanes:lanes + BLK] = low
            return carry

        lax.fori_loop(first, last, step, 0)

    settle(top_v.at[pl.ds(0, early), :, pl.ds(0, states), :], load_sem.at[1])
    convert(top_v, top_x, 0, early)
    settle(modes_v, load_sem.at[3])
    settle(tables_v.at[:, pl.ds(0, owned), :], load_sem.at[0])
    for load in small[1:]:
        load.wait()

    held = tables_v.shape[1]
    flat = tables_v.reshape(2 * states * held, states)

    def pick(delta, n):
        wanted = blocks_s[0, n] if delta == 0 else req_s[delta, 0, n]
        relative = wanted - me * owned
        inside = jnp.logical_and(relative >= 0, relative < owned)
        keep = jnp.where(inside, 1.0, 0.0).astype(F32)
        p = jnp.clip(relative, 0, owned - 1)
        left = jnp.concatenate([
            flat[pl.ds(p, states, stride=held), :],
            modes_v[0, pl.ds(p, 1), :] * -rate_s[p],
            jnp.zeros((pad - states - 1, states), F32),
        ], axis=0)
        right = flat[pl.ds(states * held + p, states, stride=held), :]
        turned = jnp.transpose(
            jnp.concatenate([left, jnp.zeros((pad, 2 * pad - states), F32)], axis=1)
        )
        scale = jnp.concatenate([
            modes_v[1, pl.ds(p, 1), :] * keep,
            jnp.full((1, 1), keep),
            jnp.zeros((1, pad - states - 1), F32),
        ], axis=1)
        gap = jnp.zeros((states, pad - states), F32)
        return jnp.concatenate([turned[0:states, :] * scale, right * keep, gap], axis=1)

    def gather(wanted, after=None):
        ready = pick(*wanted[0])
        for i, (delta, n) in enumerate(wanted):
            coming = pick(*wanted[i + 1]) if i + 1 < len(wanted) else None
            mine[delta, n, 0:sent, :] = ready
            if after is not None:
                after(delta, n)
            ready = coming

    def beside(d, n):
        pltpu.make_async_remote_copy(
            src_ref=mine.at[d, n, pl.ds(0, sent)],
            dst_ref=near_v.at[d ^ 1, n, pl.ds(0, sent)],
            send_sem=tab_send.at[1 if d == 1 else 0],
            recv_sem=near_recv.at[0] if d == 1 else pass_recv.at[(d ^ 1) - 2, n - 1],
            device_id={"dom": me ^ 1},
            device_id_type=MESH,
        ).start()

    def straight(d):
        pltpu.make_async_remote_copy(
            src_ref=mine.at[d, 0, pl.ds(0, sent)],
            dst_ref=lone.at[d, pl.ds(0, sent)],
            send_sem=lone_send.at[0],
            recv_sem=near_recv.at[1],
            device_id={"dom": me ^ d},
            device_id_type=MESH,
        ).start()

    def beyond(d, n):
        passed[d, n, 0:sent, :] = mine[d, n, 0:sent, :] + near_v[d, n, 0:sent, :]
        pltpu.make_async_remote_copy(
            src_ref=passed.at[d, n, pl.ds(0, sent)],
            dst_ref=far_v.at[d // 2, n, pl.ds(0, sent)],
            send_sem=tab_send.at[0],
            recv_sem=far_recv.at[d // 2 - 1, n - 1],
            device_id={"dom": me ^ d},
            device_id_type=MESH,
        ).start()

    others = list(reversed(range(2, doms)))
    same = [d for d in others if not d & 1]
    cross = [d for d in others if d & 1]

    def serve(order, after):
        for d in order:
            settle(req_s.at[pl.ds(d, 1)], req_recv.at[d])
            gather([(d, 0)])
            straight(d)
            gather([(d, n) for n in range(1, nblk)], after)

    pl.when(odd)(functools.partial(serve, same + cross, None))
    pl.when(jnp.logical_not(odd))(functools.partial(serve, cross + same, beside))
    settle(req_s.at[pl.ds(1, 1)], req_recv.at[1])
    gather([(1, n) for n in range(nblk)])
    for n in range(nblk):
        beside(1, n)

    @pl.when(odd)
    def _():
        for n in range(1, nblk):
            for d in (same + cross if n == 1 else cross + same):
                settle(near_v.at[pl.ds(d, 1), n, pl.ds(0, sent)], pass_recv.at[d - 2, n - 1])
                beyond(d, n)

    gather([(0, n) for n in range(nblk)])
    pl.semaphore_wait(gossip.at[0], around)
    greet(gossip.at[1])
    settle(top_v.at[pl.ds(early, nblk - early), :, pl.ds(0, states), :], load_sem.at[4])
    convert(top_v, top_x, early, nblk)
    settle(bottom_v.at[:, :, pl.ds(0, states), :], load_sem.at[2])
    convert(bottom_v, bottom_x, 0, nblk)
    settle(req_v.at[pl.ds(1, doms - 1)], req_recv.at[0])
    times = [lengths_s[chosen_s[b]] for b in range(branches)]
    for h in range(rows):
        parts_v[h, 0:2 * kinds, :] = jnp.zeros((2 * kinds, 2 * BLK), BF16)
    ones = jnp.ones((16, 2 * BLK), BF16)

    def block(n):
        tile = mine[0, n]
        tile = tile + near_v[0, n]
        if n == 0:
            for d in range(2, doms):
                tile = tile + lone[d]
        else:
            for k in range(1, doms // 2):
                tile = tile + far_v[k, n]
        l_high, l_low = split(tile[:, 0:pad])
        r_high, r_low = split(tile[:, pad:2 * pad])
        l_all = jnp.concatenate([l_high, l_high, l_low], axis=1)
        r_all = jnp.concatenate([r_high, r_high, r_low], axis=1)
        expo = jnp.broadcast_to(tile[:, states:states + 1], (pad, BLK))
        power = expo * LOG2E
        for half in range(branches // 2):
            at = n * (branches // 2) + half
            t_x = top_x[at]
            b_x = bottom_x[at]
            lefts = jnp.dot(
                l_all, jnp.concatenate([t_x, t_x[0:pad]], axis=0), preferred_element_type=F32
            )
            rights = jnp.dot(
                r_all, jnp.concatenate([b_x, b_x[0:pad]], axis=0), preferred_element_type=F32
            )
            joint = lefts * rights
            for side in range(2):
                b = 2 * half + side
                decayed = joint[:, side * BLK:(side + 1) * BLK] * jnp.exp2(power * times[b])
                once = decayed * expo
                twice = once * expo
                like_v[n % 2, 0, b:b + 1, :] = jnp.sum(decayed, axis=0, keepdims=True)
                like_v[n % 2, 1, b:b + 1, :] = jnp.sum(once, axis=0, keepdims=True)
                like_v[n % 2, 2, b:b + 1, :] = jnp.sum(twice, axis=0, keepdims=True)
        like0 = like_v[n % 2, 0]
        first_d = like_v[n % 2, 1] / like0
        second_d = like_v[n % 2, 2] / like0 - first_d * first_d
        w_sites = pattern_ref[pl.ds(n, 1), :].astype(F32)
        loglik_ref[pl.ds(n, branches, stride=nblk), :] = like0
        both = jnp.concatenate([first_d, second_d], axis=0) * w_sites
        q = group - 1 - n % group
        for i, part in enumerate(split(both)):
            parts_v[n // group, q * kinds:(q + 1) * kinds, i * BLK:(i + 1) * BLK] = part

    def sums_of(h, count):
        return lax.dot_general(
            ones,
            parts_v[h, 0:count * kinds],
            (((1,), (1,)), ((), ())),
            preferred_element_type=F32,
        )[0:1]

    def arrive(n):
        for k in range(1, doms // 2):
            settle(far_v.at[k, n, pl.ds(0, sent)], far_recv.at[k - 1, n - 1])

    settle(lone.at[pl.ds(2, doms - 2), pl.ds(0, sent)], near_recv.at[1])
    alone = nblk // 2
    pl.semaphore_wait(gossip.at[1], around)
    greet(gossip.at[2])
    for n in range(0, alone, 2):
        if n:
            arrive(n)
        else:
            settle(near_v.at[0, :, pl.ds(0, sent)], near_recv.at[0])
        arrive(n + 1)
        block(n)
        block(n + 1)
        if n == 0:
            for step in range(3, outer):
                pl.semaphore_wait(gossip.at[step - 1], around)
                greet(gossip.at[step])
        if n == 2:
            pl.semaphore_wait(gossip.at[outer - 1], around)
            for z in reversed(range(outer)):
                for x in range(inner):
                    if x or z:
                        pltpu.make_async_remote_copy(
                            src_ref=req_v,
                            dst_ref=ids_v.at[spot],
                            send_sem=ids_send.at[0],
                            recv_sem=ids_recv.at[0],
                            device_id={"site": at_site(x, z)},
                            device_id_type=MESH,
                        ).start()
            ids_v[spot] = req_v[...]

    for n in range(alone, nblk):
        arrive(n)
        if n == nblk - 2:
            for h in range(rows):
                pay_v[h:h + 1, :] = sums_of(h, group)
        block(n)
    late = min(2, group) * kinds
    pay_v[rows - 1:rows, 0:late] = sums_of(rows - 1, min(2, group))[:, 0:late]

    peers = [(d, x, z) for d in range(doms) for x in range(inner) for z in range(outer)][1:]
    peers.sort(key=lambda peer: -(max(peer[2], -peer[2] % outer) + peer[1] + peer[0] // 2))
    for d, x, z in peers:
        pltpu.make_async_remote_copy(
            src_ref=pay_v.at[pl.ds(0, rows)],
            dst_ref=pay_in.at[pl.ds(pl.multiple_of((spot * doms + d) * slot, slot), rows)],
            send_sem=pay_send.at[0],
            recv_sem=pay_recv.at[0],
            device_id={"dom": me ^ d, "site": at_site(x, z)},
            device_id_type=MESH,
        ).start()
    pay_in[pl.ds(pl.multiple_of(spot * doms * slot, slot), rows), :] = pay_v[0:rows]

    weights = pattern_ref[...].astype(F32)
    for b in range(branches):
        lines = pl.ds(b * nblk, nblk)
        loglik_ref[lines, :] = weights * jnp.log(loglik_ref[lines, :])
    settle(ids_v.at[pl.ds(1, sites - 1)], ids_recv.at[0])
    ids = ids_v[...].reshape(sites * doms, BLK)
    lane = lax.broadcasted_iota(jnp.int32, (sites * doms, BLK), 1)
    for n in range(nblk):
        hit = jnp.logical_and(ids[:, n:n + 1] - me * owned == lane, lane < owned)
        start = (n // group) * sites * doms
        hot_v[group - 1 - n % group, start:start + sites * doms, 0:BLK] = (
            jnp.where(hit, 1.0, 0.0).astype(BF16)
        )
    hot_v[:, :, BLK:2 * BLK] = jnp.ones((group, rows * sites * doms, BLK), BF16)
    row = lax.broadcasted_iota(jnp.int32, (branches, BLK), 0)
    old = jnp.zeros((branches, BLK), F32)
    for b in range(branches):
        old = jnp.where(row == b, times[b], old)
    old_v[...] = old
    tree = new_ref.shape[1]
    place = lax.broadcasted_iota(jnp.int32, (1, tree), 1)
    kept = row_v[...]
    for b in range(branches):
        here = place == chosen_s[b]
        pick_v[b:b + 1, :] = jnp.where(here, 1.0, 0.0)
        kept = jnp.where(here, 0.0, kept)
    row_v[...] = kept

    settle(pay_in.at[pl.ds(0, (sites * doms - 1) * rows)], pay_recv.at[0])
    lines = jnp.concatenate([pay_in[pl.ds(h, sites * doms, stride=slot), :] for h in range(rows)], axis=0)
    flipped = jnp.transpose(lines)
    stacked = jnp.zeros((3 * kinds, 2 * BLK), F32)
    for q in range(group):
        third = thirds(flipped[q * kinds:(q + 1) * kinds, :])
        stacked = stacked + jnp.dot(
            jnp.concatenate(third, axis=0), hot_v[q], preferred_element_type=F32
        )
    total = stacked[0:kinds] + stacked[kinds:2 * kinds] + stacked[2 * kinds:3 * kinds]
    share_ref[...] = total[:, 0:owned]
    sums = total[:, BLK:2 * BLK]
    value = old_v[...] - sums[0:branches] / sums[branches:kinds]
    for start in range(0, tree, BLK):
        width = min(BLK, tree - start)
        lanes = slice(start, start + width)
        chosen = jnp.where(pick_v[:, lanes] > 0.0, value[:, 0:width], 0.0)
        new_ref[:, lanes] = row_v[:, lanes] + jnp.sum(chosen, axis=0, keepdims=True)

    for kind in range(2):
        settle(req_v.at[pl.ds(1, doms - 1)], req_send.at[kind])
    settle(ids_v.at[pl.ds(1, sites - 1)], ids_send.at[0])
    settle(pay_in.at[pl.ds(0, (sites * doms - 1) * rows)], pay_send.at[0])
    settle(lone.at[pl.ds(2, doms - 2), pl.ds(0, sent)], lone_send.at[0])
    settle(
        mine.at[pl.ds(2, doms - 2), pl.ds(1, nblk - 1), pl.ds(0, sent)], tab_send.at[0]
    )
    settle(mine.at[1, :, pl.ds(0, sent)], tab_send.at[1])


def store(loglik_v, share_v, new_v, loglik_ref, share_ref, new_ref, sem):
    copies = [
        pltpu.make_async_copy(source, dest, sem.at[i])
        for i, (source, dest) in enumerate((
            (new_v, new_ref), (share_v, share_ref), (loglik_v, loglik_ref)
        ))
    ]
    for copy in copies:
        copy.start()
    for copy in copies:
        copy.wait()


def on_device(
    top_partial,
    bottom_partial,
    left_vectors,
    right_vectors,
    decay_rates,
    state_weights,
    part_rates,
    branch_lengths,
    pattern_weights,
    block_partition,
    chosen_branches,
):
    doms = lax.axis_size("dom")
    sites = lax.axis_size("site")
    branches, states, _, sites_here = top_partial.shape
    nblk = sites_here // BLK
    owned = left_vectors.shape[0]
    tree = branch_lengths.shape[0]
    pad = round_up(states + 2, 64)
    inner = 2 if sites % 2 == 0 else 1
    outer = sites // inner
    held = round_up(owned, 8) + 8
    kinds = 2 * branches
    group = BLK // kinds
    rows = nblk // group
    cfg = (doms, sites, inner, branches, states, nblk, owned, pad, group)
    hbm = pl.BlockSpec(memory_space=pltpu.HBM)
    vmem = pl.BlockSpec(memory_space=pltpu.VMEM)
    tile = (pad, 2 * pad)
    dma = pltpu.SemaphoreType.DMA
    pattern = pattern_weights.reshape(nblk, BLK)
    loglik, share, new = pl.pallas_call(
        functools.partial(body, cfg),
        out_shape=(
            pltpu.VMEM((branches * nblk, BLK), F32),
            pltpu.VMEM((kinds, owned), F32),
            pltpu.VMEM((1, tree), F32),
        ),
        in_specs=[hbm] * 12,
        out_specs=(vmem, vmem, vmem),
        scratch_shapes=[
            pltpu.VMEM((nblk, branches, pad, BLK), F32),
            pltpu.VMEM((nblk, branches, pad, BLK), F32),
            pltpu.VMEM((2 * states, held, states), F32),
            pltpu.VMEM((doms, 1, BLK), jnp.int32),
            pltpu.SMEM((doms, 1, BLK), jnp.int32),
            pltpu.VMEM((doms, nblk) + tile, F32),
            pltpu.VMEM((doms, nblk) + tile, F32),
            pltpu.VMEM((doms, nblk) + tile, F32),
            pltpu.VMEM((doms // 2, nblk) + tile, F32),
            pltpu.VMEM((doms,) + tile, F32),
            pltpu.VMEM((nblk * branches // 2, 2 * pad, 2 * BLK), BF16),
            pltpu.VMEM((nblk * branches // 2, 2 * pad, 2 * BLK), BF16),
            pltpu.VMEM((2, 3, branches, BLK), F32),
            pltpu.VMEM((rows, group * kinds, 2 * BLK), BF16),
            pltpu.VMEM((round_up(rows, 8), BLK), F32),
            pltpu.VMEM((sites * doms * round_up(rows, 8), BLK), F32),
            pltpu.VMEM((sites, doms, 1, BLK), jnp.int32),
            pltpu.VMEM((group, rows * sites * doms, 2 * BLK), BF16),
            pltpu.VMEM((branches, BLK), F32),
            pltpu.VMEM((branches, tree), F32),
            pltpu.VMEM((1, tree), F32),
            pltpu.VMEM((2, owned, states), F32),
            pltpu.SMEM((owned,), F32),
            pltpu.SMEM((tree,), F32),
            pltpu.SMEM((branches,), jnp.int32),
            pltpu.VMEM((nblk, BLK), jnp.int32),
            pltpu.SMEM((1, nblk), jnp.int32),
            pltpu.VMEM((1, nblk), jnp.int32),
            dma((5,)),
            dma((7,)),
            pltpu.SemaphoreType.REGULAR((outer,)),
            dma((2,)),
            dma((doms,)),
            dma((2,)),
            dma((1,)),
            dma((2,)),
            dma((doms - 2, nblk - 1)),
            dma((doms // 2 - 1, nblk - 1)),
            dma((1,)),
            dma((1,)),
            dma((1,)),
            dma((1,)),
        ],
        compiler_params=pltpu.CompilerParams(
            collective_id=0, has_side_effects=True, vmem_limit_bytes=56 * 1024 * 1024
        ),
    )(
        top_partial.reshape(branches, states, nblk, BLK),
        bottom_partial.reshape(branches, states, nblk, BLK),
        jnp.swapaxes(left_vectors, 0, 1),
        jnp.swapaxes(right_vectors, 0, 1),
        decay_rates,
        state_weights,
        part_rates,
        branch_lengths,
        chosen_branches,
        pattern,
        block_partition,
        branch_lengths.reshape(1, tree),
    )
    loglik, share, new = pl.pallas_call(
        store,
        out_shape=(
            jax.ShapeDtypeStruct((branches * nblk, BLK), F32),
            jax.ShapeDtypeStruct((kinds, owned), F32),
            jax.ShapeDtypeStruct((1, tree), F32),
        ),
        in_specs=[vmem] * 3,
        out_specs=[hbm] * 3,
        scratch_shapes=[dma((3,))],
        compiler_params=pltpu.CompilerParams(vmem_limit_bytes=1024 * 1024),
    )(loglik, share, new)
    return (
        loglik.reshape(branches, 1, sites_here),
        share.reshape(2, branches, owned),
        new.reshape(tree),
    )


def solution(mesh):
    return jax.shard_map(
        on_device,
        mesh=mesh,
        in_specs=(
            P(None, None, "dom", "site"),
            P(None, None, "dom", "site"),
            P("dom", None, None),
            P("dom", None, None),
            P("dom", None),
            P("dom", None),
            P("dom"),
            P(),
            P("dom", "site"),
            P("dom", "site"),
            P(),
        ),
        out_specs=(P(None, "dom", "site"), P(None, None, "dom"), P()),
        check_vma=False,
    )
```
